16 devices in a mesh: dp: 2 (over z), tp: 8 (over y, x, core).
Axes of the slice: x: 2, y: 2, z: 2, core: 2. Of those that a mesh axis runs over, the one named last changes fastest.
Arguments:
- x_in: bfloat16 [2, 2048, 2304], P('dp', 'tp'), parts along dimension 0
- x_mid: bfloat16 [2, 2048, 2304], P('dp', 'tp'), parts along dimension 0
- d_out: bfloat16 [2, 2048, 2304], P('dp', 'tp'), parts along dimension 0
- q_saved: bfloat16 [2, 2048, 24, 96], P('dp', None, 'tp'), parts along dimension 0
- k_saved: bfloat16 [2, 2048, 24, 96], P('dp', None, 'tp'), parts along dimension 0
- v_saved: bfloat16 [2, 2048, 24, 96], P('dp', None, 'tp'), parts along dimension 0
- z_saved: bfloat16 [2, 2048, 9216], P('dp', None, 'tp'), parts along dimension 0
- ln1_gain: float32 [2304], replicated
- ln1_bias: float32 [2304], replicated
- ln2_gain: float32 [2304], replicated
- ln2_bias: float32 [2304], replicated
- w_qkv: bfloat16 [3, 2304, 24, 96], P(None, None, 'tp')
- w_proj: bfloat16 [24, 96, 2304], P('tp')
- w_fc1: bfloat16 [2304, 9216], P(None, 'tp')
- w_fc2: bfloat16 [9216, 2304], P('tp')
Outputs:
- output 1: bfloat16 [2, 2048, 2304], P('dp', 'tp'), parts along dimension 0
- output 2: float32 [6, 2304, 24, 96], P('dp', None, 'tp'), parts along dimension 0
- output 3: float32 [6, 24, 96], P('dp', 'tp'), parts along dimension 0
- output 4: float32 [48, 96, 2304], P(('dp', 'tp')), parts along dimension 0
- output 5: float32 [4608, 9216], P('dp', 'tp'), parts along dimension 0
- output 6: float32 [18432], P(('dp', 'tp')), parts along dimension 0
- output 7: float32 [18432, 2304], P(('dp', 'tp')), parts along dimension 0
- output 8: float32 [12, 2304], P('dp'), parts along dimension 0
There are 2 independent parts. The reference program is written for one: setup_inputs(seed, part) draws one part's arguments, and reference() takes and returns one part's arrays. A program takes and returns all parts, laid end to end along the dimension named above; an argument that names none is the same for every part.
All inputs are finite; a program needn't handle non-finite values.
Results may differ from the reference program's by a relative error of at most 0.0111809.
Values are sent between devices in bfloat16 or wider.
A program may use at most 1 GiB of HBM per device.

```python
import jax
import jax.numpy as jnp
from jax import lax

BATCH_SEQS = 1
SEQ_LEN = 2048
D_MODEL = 2304
N_HEADS = 24
HEAD_DIM = 96
FF_DIM = 9216
LN_EPS = 1e-5
GELU_COEF = 0.044715
GELU_SCALE = 0.7978845608028654


def draw_normal(key, shape, scale):
    return (scale * jax.random.normal(key, shape, jnp.float32)).astype(jnp.bfloat16)


def setup_inputs(seed: int = 0, part: int = 0) -> dict:
    part_keys = jax.random.split(jax.random.fold_in(jax.random.key(seed), part), 7)
    shared_keys = jax.random.split(jax.random.key(seed + 1), 8)
    tok_shape = (BATCH_SEQS, SEQ_LEN, D_MODEL)
    head_shape = (BATCH_SEQS, SEQ_LEN, N_HEADS, HEAD_DIM)
    return {
        'x_in': draw_normal(part_keys[0], tok_shape, 1.0),
        'x_mid': draw_normal(part_keys[1], tok_shape, 1.0),
        'd_out': draw_normal(part_keys[2], tok_shape, 1.0),
        'q_saved': draw_normal(part_keys[3], head_shape, 1.0),
        'k_saved': draw_normal(part_keys[4], head_shape, 1.0),
        'v_saved': draw_normal(part_keys[5], head_shape, 1.0),
        'z_saved': draw_normal(part_keys[6], (BATCH_SEQS, SEQ_LEN, FF_DIM), 1.5),
        'ln1_gain': jax.random.uniform(shared_keys[0], (D_MODEL,), jnp.float32, 0.5, 1.5),
        'ln1_bias': 0.5 * jax.random.normal(shared_keys[1], (D_MODEL,), jnp.float32),
        'ln2_gain': jax.random.uniform(shared_keys[2], (D_MODEL,), jnp.float32, 0.5, 1.5),
        'ln2_bias': 0.5 * jax.random.normal(shared_keys[3], (D_MODEL,), jnp.float32),
        'w_qkv': draw_normal(shared_keys[4], (3, D_MODEL, N_HEADS, HEAD_DIM), D_MODEL ** -0.5),
        'w_proj': draw_normal(shared_keys[5], (N_HEADS, HEAD_DIM, D_MODEL), D_MODEL ** -0.5),
        'w_fc1': draw_normal(shared_keys[6], (D_MODEL, FF_DIM), D_MODEL ** -0.5),
        'w_fc2': draw_normal(shared_keys[7], (FF_DIM, D_MODEL), FF_DIM ** -0.5),
    }


def layer_norm_fwd(token_rows, norm_gain, norm_bias):
    rows_f32 = token_rows.astype(jnp.float32)
    centered = rows_f32 - jnp.mean(rows_f32, axis=-1, keepdims=True)
    inv_std = lax.rsqrt(jnp.mean(centered * centered, axis=-1, keepdims=True) + LN_EPS)
    x_hat = centered * inv_std
    return x_hat, inv_std, (x_hat * norm_gain + norm_bias).astype(jnp.bfloat16)


def layer_norm_bwd(grad_norm, x_hat, inv_std, norm_gain):
    grad_hat = grad_norm * norm_gain
    centered_grad = grad_hat - jnp.mean(grad_hat, axis=-1, keepdims=True)
    return inv_std * (centered_grad - x_hat * jnp.mean(grad_hat * x_hat, axis=-1, keepdims=True))


def gelu_parts(pre_act):
    tanh_val = jnp.tanh(GELU_SCALE * (pre_act + GELU_COEF * pre_act * pre_act * pre_act))
    act_value = 0.5 * pre_act * (1.0 + tanh_val)
    act_slope = 0.5 * (1.0 + tanh_val) + 0.5 * pre_act * (1.0 - tanh_val * tanh_val) * GELU_SCALE * (1.0 + 3.0 * GELU_COEF * pre_act * pre_act)
    return act_value, act_slope


def head_attention_grads(operands):
    q_head, k_head, v_head, dctx_head = operands
    score_scale = HEAD_DIM ** -0.5
    q_wide = q_head.astype(jnp.float32)
    k_wide = k_head.astype(jnp.float32)
    v_wide = v_head.astype(jnp.float32)
    dctx_wide = dctx_head.astype(jnp.float32)
    scores = jnp.einsum('bqe,bke->bqk', q_wide, k_wide) * score_scale
    row_ids = lax.broadcasted_iota(jnp.int32, (SEQ_LEN, SEQ_LEN), 0)
    col_ids = lax.broadcasted_iota(jnp.int32, (SEQ_LEN, SEQ_LEN), 1)
    scores = jnp.where(row_ids >= col_ids, scores, -1e30)
    attn_probs = jax.nn.softmax(scores, axis=-1)
    probs_low = attn_probs.astype(jnp.bfloat16).astype(jnp.float32)
    context = jnp.einsum('bqk,bke->bqe', probs_low, v_wide).astype(jnp.bfloat16)
    grad_probs = jnp.einsum('bqe,bke->bqk', dctx_wide, v_wide)
    grad_scores = attn_probs * (grad_probs - jnp.sum(grad_probs * attn_probs, axis=-1, keepdims=True)) * score_scale
    scores_low = grad_scores.astype(jnp.bfloat16).astype(jnp.float32)
    grad_q = jnp.einsum('bqk,bke->bqe', scores_low, k_wide).astype(jnp.bfloat16)
    grad_k = jnp.einsum('bqk,bqe->bke', scores_low, q_wide).astype(jnp.bfloat16)
    grad_v = jnp.einsum('bqk,bqe->bke', probs_low, dctx_wide).astype(jnp.bfloat16)
    return context, grad_q, grad_k, grad_v


def reference(x_in, x_mid, d_out, q_saved, k_saved, v_saved, z_saved, ln1_gain, ln1_bias, ln2_gain, ln2_bias, w_qkv, w_proj, w_fc1, w_fc2):
    n_tok = BATCH_SEQS * SEQ_LEN
    norm2_hat, norm2_rstd, h2_norm = layer_norm_fwd(x_mid, ln2_gain, ln2_bias)
    act_value, act_slope = gelu_parts(z_saved.astype(jnp.float32))
    dout_rows = d_out.reshape(n_tok, D_MODEL)
    grad_wfc2 = jnp.dot(act_value.astype(jnp.bfloat16).reshape(n_tok, FF_DIM).T, dout_rows, preferred_element_type=jnp.float32)
    grad_act = jnp.dot(dout_rows, w_fc2.T, preferred_element_type=jnp.float32)
    grad_pre = (grad_act * act_slope.reshape(n_tok, FF_DIM)).astype(jnp.bfloat16)
    grad_wfc1 = jnp.dot(h2_norm.reshape(n_tok, D_MODEL).T, grad_pre, preferred_element_type=jnp.float32)
    grad_bfc1 = jnp.sum(grad_pre.astype(jnp.float32), axis=0)
    grad_h2 = jnp.dot(grad_pre, w_fc1.T, preferred_element_type=jnp.float32).reshape(BATCH_SEQS, SEQ_LEN, D_MODEL)
    grad_mid = (d_out.astype(jnp.float32) + layer_norm_bwd(grad_h2, norm2_hat, norm2_rstd, ln2_gain)).astype(jnp.bfloat16)
    mid_rows = grad_mid.reshape(n_tok, D_MODEL)
    grad_ctx = jnp.dot(mid_rows, w_proj.reshape(D_MODEL, D_MODEL).T, preferred_element_type=jnp.float32).astype(jnp.bfloat16)
    grad_ctx = grad_ctx.reshape(BATCH_SEQS, SEQ_LEN, N_HEADS, HEAD_DIM)
    context, grad_q, grad_k, grad_v = lax.map(head_attention_grads, (jnp.moveaxis(q_saved, 2, 0), jnp.moveaxis(k_saved, 2, 0), jnp.moveaxis(v_saved, 2, 0), jnp.moveaxis(grad_ctx, 2, 0)))
    context_rows = jnp.moveaxis(context, 0, 2).reshape(n_tok, D_MODEL)
    grad_wproj = jnp.dot(context_rows.T, mid_rows, preferred_element_type=jnp.float32).reshape(N_HEADS, HEAD_DIM, D_MODEL)
    norm1_hat, norm1_rstd, h1_norm = layer_norm_fwd(x_in, ln1_gain, ln1_bias)
    qkv_rows = jnp.moveaxis(jnp.stack([grad_q, grad_k, grad_v]), 1, 3).reshape(3, n_tok, D_MODEL).astype(jnp.float32)
    grad_wqkv = jnp.einsum('td,ite->ide', h1_norm.reshape(n_tok, D_MODEL).astype(jnp.float32), qkv_rows).reshape(3, D_MODEL, N_HEADS, HEAD_DIM)
    grad_bqkv = jnp.sum(qkv_rows, axis=1).reshape(3, N_HEADS, HEAD_DIM)
    grad_h1 = jnp.einsum('ite,ide->td', qkv_rows, w_qkv.reshape(3, D_MODEL, D_MODEL).astype(jnp.float32)).reshape(BATCH_SEQS, SEQ_LEN, D_MODEL)
    grad_x = (grad_mid.astype(jnp.float32) + layer_norm_bwd(grad_h1, norm1_hat, norm1_rstd, ln1_gain)).astype(jnp.bfloat16)
    grad_vecs = jnp.stack([
        jnp.sum(grad_h1 * norm1_hat, axis=(0, 1)),
        jnp.sum(grad_h1, axis=(0, 1)),
        jnp.sum(grad_h2 * norm2_hat, axis=(0, 1)),
        jnp.sum(grad_h2, axis=(0, 1)),
        jnp.sum(grad_mid.astype(jnp.float32), axis=(0, 1)),
        jnp.sum(d_out.astype(jnp.float32), axis=(0, 1)),
    ])
    return grad_x, grad_wqkv, grad_bqkv, grad_wproj, grad_wfc1, grad_bfc1, grad_wfc2, grad_vecs
```

```python
import jax, jax.numpy as jnp
from jax import lax
from jax.experimental import pallas as pl
from jax.experimental.pallas import tpu as pltpu
from jax.sharding import PartitionSpec as P
T=2048; E=96; NH=3; BQ=512; NQ=T//BQ; BLK=256
C=E**-0.5; C2=C*1.4426950408889634
f32=jnp.float32; bf16=jnp.bfloat16

def rel_pos(block, me):
    j=lax.bitwise_xor(block, me)
    return lax.shift_right_logical(j,1)+4*lax.bitwise_and(j,1)

def tn(a,b,ca,cb): return lax.dot_general(a,b,(((ca,),(cb,)),((),())),preferred_element_type=f32)

def fold8(a): return jnp.sum(a.reshape(a.shape[0]//8,8,a.shape[1]),axis=0)
def foldmax8(a): return jnp.max(a.reshape(a.shape[0]//8,8,a.shape[1]),axis=0)

def causal(s, fill):
    r=lax.broadcasted_iota(jnp.int32,s.shape,0); c=lax.broadcasted_iota(jnp.int32,s.shape,1)
    return jnp.where(r<=c,s,fill)

def fwd_kernel(me_ref,q_ref,k_ref,v_ref,ctx_ref,lse_ref,kt,sc,acc):
    i=pl.program_id(1)
    @pl.when(i==0)
    def _(): kt[...]=k_ref[0].T
    q=q_ref[0]
    def rows(j): return pl.ds(pl.multiple_of(j*BQ,BQ),BQ)
    def p1(j,m):
        s=jnp.dot(kt[rows(j),:],q,preferred_element_type=f32)
        sc[rows(j),:]=s
        return jnp.maximum(m,foldmax8(s))
    m=lax.fori_loop(0,i,p1,jnp.full((8,BQ),-1e30,f32))
    s=causal(jnp.dot(kt[rows(i),:],q,preferred_element_type=f32),-1e30)
    sc[rows(i),:]=s
    m=jnp.max(jnp.maximum(m,foldmax8(s)),axis=0,keepdims=True)*C2
    def p2(j,l):
        e=jnp.exp2(sc[rows(j),:]*C2-m)
        sc[rows(j),:]=e
        return l+fold8(e)
    l=jnp.sum(lax.fori_loop(0,i+1,p2,jnp.zeros((8,BQ),f32)),axis=0,keepdims=True)
    inv=1.0/l
    lse_ref[0]=m+jnp.log2(l)
    acc[...]=jnp.zeros_like(acc)
    def p3(j,_):
        p=(sc[rows(j),:]*inv).astype(bf16)
        acc[...]+=jnp.dot(v_ref[0,:,rows(j)],p,preferred_element_type=f32)
        return 0
    lax.fori_loop(0,i+1,p3,0)
    for a in range(BQ//BLK):
        pos=rel_pos(i*(BQ//BLK)+a,me_ref[0])
        ctx_ref[0,:,pl.ds(pl.multiple_of(pos*BLK,BLK),BLK)]=acc[:,a*BLK:(a+1)*BLK].astype(bf16)

def bwd_kernel(me_ref,q_ref,k_ref,v_ref,g_ref,lse_ref,out_ref,kt,vt,psc,dsc,g_sc,dq,dk,dv):
    i=pl.program_id(1)
    @pl.when(i==0)
    def _():
        kt[...]=k_ref[0].T
        vt[...]=v_ref[0].T
        dk[...]=jnp.zeros_like(dk); dv[...]=jnp.zeros_like(dv)
    def rows(j): return pl.ds(pl.multiple_of(j*BQ,BQ),BQ)
    for a in range(BQ//BLK):
        pos=rel_pos(i*(BQ//BLK)+a,me_ref[0])
        g_sc[:,a*BLK:(a+1)*BLK]=g_ref[0,:,pl.ds(pl.multiple_of(pos*BLK,BLK),BLK)]
    q=q_ref[0]; g=g_sc[...]; lse=lse_ref[0]
    def tile(j,d,diag):
        s=jnp.dot(kt[rows(j),:],q,preferred_element_type=f32)
        p=jnp.exp2(s*C2-lse)
        if diag: p=causal(p,0.0)
        dp=jnp.dot(vt[rows(j),:],g,preferred_element_type=f32)
        psc[rows(j),:]=p; dsc[rows(j),:]=dp
        return d+fold8(p*dp)
    d=lax.fori_loop(0,i,lambda j,d: tile(j,d,False),jnp.zeros((8,BQ),f32))
    delta=jnp.sum(tile(i,d,True),axis=0,keepdims=True)
    dq[...]=jnp.zeros_like(dq)
    def p2(j,_):
        p=psc[rows(j),:]
        ds=(p*(dsc[rows(j),:]-delta)*C).astype(bf16)
        dq[...]+=jnp.dot(k_ref[0,:,rows(j)],ds,preferred_element_type=f32)
        dk[:,rows(j)]+=tn(q,ds,1,1)
        dv[:,rows(j)]+=tn(g,p.astype(bf16),1,1)
        return 0
    lax.fori_loop(0,i+1,p2,0)
    for a in range(BQ//BLK):
        pos=rel_pos(i*(BQ//BLK)+a,me_ref[0])
        out_ref[0,0,:,pl.ds(pl.multiple_of(pos*BLK,BLK),BLK)]=dq[:,a*BLK:(a+1)*BLK].astype(bf16)
    @pl.when(i==NQ-1)
    def _():
        for b in range(T//BLK):
            at=pl.ds(pl.multiple_of(rel_pos(b,me_ref[0])*BLK,BLK),BLK)
            out_ref[1,0,:,at]=dk[:,b*BLK:(b+1)*BLK].astype(bf16)
            out_ref[2,0,:,at]=dv[:,b*BLK:(b+1)*BLK].astype(bf16)

full=lambda: pl.BlockSpec((1,E,T),lambda h,i,me:(h,0,0))
qblk=lambda: pl.BlockSpec((1,E,BQ),lambda h,i,me:(h,0,i))
lblk=lambda: pl.BlockSpec((1,1,BQ),lambda h,i,me:(h,0,i))
NEL=NH*(NQ*(NQ+1)//2)*BQ*BQ
def attn_fwd(me,q,k,v):
    return pl.pallas_call(fwd_kernel,name="attn_fwd",
        grid_spec=pltpu.PrefetchScalarGridSpec(num_scalar_prefetch=1,grid=(NH,NQ),
            in_specs=[qblk(),full(),full()],out_specs=[full(),lblk()],
            scratch_shapes=[pltpu.VMEM((T,E),bf16),pltpu.VMEM((T,BQ),f32),pltpu.VMEM((E,BQ),f32)]),
        out_shape=[jax.ShapeDtypeStruct((NH,E,T),bf16),jax.ShapeDtypeStruct((NH,1,T),f32)],
        compiler_params=pltpu.CompilerParams(dimension_semantics=("arbitrary","arbitrary"),vmem_limit_bytes=40<<20),
        cost_estimate=pl.CostEstimate(flops=NEL*512*2,bytes_accessed=8<<20,transcendentals=NEL))(me,q,k,v)
def attn_bwd(me,q,k,v,g,lse):
    return pl.pallas_call(bwd_kernel,name="attn_bwd",
        grid_spec=pltpu.PrefetchScalarGridSpec(num_scalar_prefetch=1,grid=(NH,NQ),
            in_specs=[qblk(),full(),full(),full(),lblk()],
            out_specs=pl.BlockSpec((3,1,E,T),lambda h,i,me:(0,h,0,0)),
            scratch_shapes=[pltpu.VMEM((T,E),bf16),pltpu.VMEM((T,E),bf16),pltpu.VMEM((T,BQ),f32),pltpu.VMEM((T,BQ),f32),
                pltpu.VMEM((E,BQ),bf16),pltpu.VMEM((E,BQ),f32),pltpu.VMEM((E,T),f32),pltpu.VMEM((E,T),f32)]),
        out_shape=jax.ShapeDtypeStruct((3,NH,E,T),bf16),
        compiler_params=pltpu.CompilerParams(dimension_semantics=("arbitrary","arbitrary"),vmem_limit_bytes=48<<20),
        cost_estimate=pl.CostEstimate(flops=NEL*1024*2,bytes_accessed=12<<20,transcendentals=NEL))(me,q,k,v,g,lse)

LN_EPS=1e-5
GELU_COEF=0.044715
GELU_SCALE=0.7978845608028654
D=2304
ORDER=(0,2,4,6,1,3,5,7)

def hop(a, k):
    return lax.ppermute(a, 'tp', [(i, i ^ k) for i in range(8)])

def gather(block):
    half=block.shape[0]//2
    from_x, from_y = hop(block, 2), hop(block, 4)
    d0 = hop(from_x[:half], 4)
    d1 = hop(from_y[half:], 2)
    mine=[block, from_x, from_y, d0, d1]
    other=[hop(p, 1) for p in mine]
    return jnp.concatenate(mine+other, axis=0)

def scatter(partial_fn):
    other = hop(partial_fn(1024, 2048, None), 1)
    mine = partial_fn(0, 1024, other)
    own, xb, yb, db = (mine[256*i:256*(i+1)] for i in range(4))
    r0 = hop(db[:128], 2)
    r1 = hop(db[128:], 4)
    x0 = hop(xb[:128], 2)
    y1 = hop(yb[128:], 4)
    y0 = hop((yb[:128].astype(f32)+r0.astype(f32)).astype(bf16), 4)
    x1 = hop((xb[128:].astype(f32)+r1.astype(f32)).astype(bf16), 2)
    return own, x0, x1, y0, y1

def layer_norm_fwd(token_rows, norm_gain, norm_bias):
    rows_f32 = token_rows.astype(f32)
    centered = rows_f32 - jnp.mean(rows_f32, axis=-1, keepdims=True)
    inv_std = lax.rsqrt(jnp.mean(centered * centered, axis=-1, keepdims=True) + LN_EPS)
    return (centered * inv_std * norm_gain + norm_bias).astype(bf16)

def ln_bwd_kernel(own, x0, x1, y0, y1, rows, skip, gain, out, vec):
    i=pl.program_id(0)
    dh=own[...].astype(f32)+jnp.where(i<4, x0[...], x1[...]).astype(f32)+jnp.where(i<4, y0[...], y1[...]).astype(f32)
    r=rows[...].astype(f32)
    cen=r-jnp.mean(r,axis=-1,keepdims=True)
    rstd=lax.rsqrt(jnp.mean(cen*cen,axis=-1,keepdims=True)+LN_EPS)
    hat=cen*rstd
    gh=dh*gain[...]
    cg=gh-jnp.mean(gh,axis=-1,keepdims=True)
    sk=skip[...].astype(f32)
    o=(sk+rstd*(cg-hat*jnp.mean(gh*hat,axis=-1,keepdims=True))).astype(bf16)
    out[...]=o
    @pl.when(i==0)
    def _(): vec[...]=jnp.zeros_like(vec)
    add=lambda k,a: vec.__setitem__(k, vec[k]+fold8(a))
    add(0, dh*hat); add(1, dh); add(2, o.astype(f32)); add(3, sk)

def ln_bwd(parts, rows, skip, gain, name):
    R=32
    blk=pl.BlockSpec((R,D),lambda i:(i,0))
    lo=pl.BlockSpec((R,D),lambda i:(jnp.minimum(i,3),0))
    hi=pl.BlockSpec((R,D),lambda i:(jnp.maximum(i-4,0),0))
    out,vec=pl.pallas_call(ln_bwd_kernel,name=name,grid=(8,),
        in_specs=[blk,lo,hi,lo,hi,blk,blk,pl.BlockSpec((1,D),lambda i:(0,0))],
        out_specs=[blk,pl.BlockSpec((4,8,D),lambda i:(0,0,0))],
        out_shape=[jax.ShapeDtypeStruct((256,D),bf16),jax.ShapeDtypeStruct((4,8,D),f32)],
        compiler_params=pltpu.CompilerParams(dimension_semantics=("arbitrary",)),
        cost_estimate=pl.CostEstimate(flops=256*D*40,bytes_accessed=6<<20,transcendentals=0))(*parts,rows,skip,gain.reshape(1,D))
    return out,jnp.sum(vec,axis=1)

def all_sum(a):
    for k in (1,2,4):
        a=a+hop(a,k)
    return a

def solution(mesh):
    def local(x_in, x_mid, d_out, q_saved, k_saved, v_saved, z_saved, g1, b1, g2, b2, w_qkv, w_proj, w_fc1, w_fc2):
        me=lax.axis_index('tp')
        me1=jnp.reshape(me,(1,)).astype(jnp.int32)
        x_in, x_mid, d_out, z = x_in[0], x_mid[0], d_out[0], z_saved[0]
        heads=lambda a: a[0].transpose(1,2,0)
        q,k,v=heads(q_saved),heads(k_saved),heads(v_saved)
        wqkv=w_qkv.transpose(0,2,3,1).reshape(3*NH*E,D)
        wo=w_proj.reshape(NH*E,D)
        dy=gather(d_out)
        ctx,lse=attn_fwd(me1,q,k,v)
        ctx=ctx.reshape(NH*E,T)
        zr=jnp.concatenate([lax.dynamic_slice_in_dim(z,lax.bitwise_xor(me,j)*256,256,0) for j in ORDER],axis=0)
        zf=zr.astype(f32)
        th=jnp.tanh(GELU_SCALE*(zf+GELU_COEF*zf*zf*zf))
        u=(0.5*zf*(1.0+th)).astype(bf16)
        slope=0.5*(1.0+th)+0.5*zf*(1.0-th*th)*GELU_SCALE*(1.0+3.0*GELU_COEF*zf*zf)
        u,slope=lax.optimization_barrier((u,slope))
        h2=gather(layer_norm_fwd(x_mid,g2,b2))
        dz=(tn(dy,w_fc2,1,1)*slope).astype(bf16)
        def part2(lo,hi,extra):
            a=tn(dz[lo:hi],w_fc1,1,1)
            return (a if extra is None else a.astype(bf16).astype(f32)+extra.astype(f32)).astype(bf16)
        mid,vec2=ln_bwd(scatter(part2),x_mid,d_out,g2,"ln2_bwd")
        grad_wfc2=tn(u,dy,0,0)
        grad_wfc1=tn(h2,dz,0,0)
        grad_bfc1=jnp.sum(dz,axis=0,dtype=f32)
        dx1=gather(mid)
        h1=gather(layer_norm_fwd(x_in,g1,b1))
        dctx=tn(wo,dx1,1,1).astype(bf16).reshape(NH,E,T)
        dqkv=attn_bwd(me1,q,k,v,dctx,lse).reshape(3*NH*E,T)
        def part1(lo,hi,extra):
            a=tn(dqkv[:,lo:hi],wqkv,0,0)
            return (a if extra is None else a.astype(bf16).astype(f32)+extra.astype(f32)).astype(bf16)
        dx,vec1=ln_bwd(scatter(part1),x_in,mid,g1,"ln1_bwd")
        grad_wproj=jnp.dot(ctx,dx1,preferred_element_type=f32).reshape(NH,E,D)
        grad_wqkv=jnp.dot(dqkv,h1,preferred_element_type=f32).reshape(3,NH,E,D).transpose(0,3,1,2)
        grad_bqkv=jnp.sum(dqkv,axis=1,dtype=f32).reshape(3,NH,E)
        lo=all_sum(vec2); hi=all_sum(vec1[:2])
        grad_vecs=jnp.concatenate([hi,lo],axis=0)
        return dx[None], grad_wqkv, grad_bqkv, grad_wproj, grad_wfc1, grad_bfc1, grad_wfc2, grad_vecs

    tok_spec = P('dp', 'tp', None)
    head_spec = P('dp', None, 'tp', None)
    in_specs = (tok_spec, tok_spec, tok_spec, head_spec, head_spec, head_spec, P('dp', None, 'tp'),
                P(None), P(None), P(None), P(None),
                P(None, None, 'tp', None), P('tp', None, None), P(None, 'tp'), P('tp', None))
    out_specs = (tok_spec, P('dp', None, 'tp', None), P('dp', 'tp', None), P(('dp', 'tp'), None, None),
                 P('dp', 'tp'), P(('dp', 'tp')), P(('dp', 'tp'), None), P('dp', None))
    return jax.shard_map(local, mesh=mesh, in_specs=in_specs, out_specs=out_specs, check_vma=False)
```

```python
import jax, jax.numpy as jnp
from jax import lax
from jax.experimental import pallas as pl
from jax.experimental.pallas import tpu as pltpu
from jax.sharding import PartitionSpec as P
T=2048; E=96; NH=3; BQ=512; NQ=T//BQ; BLK=256
C=E**-0.5; C2=C*1.4426950408889634
f32=jnp.float32; bf16=jnp.bfloat16

def turn(h, core):
    return jnp.where(core==0, h, (h%2)*2+h//2)

def rel_pos(block, me):
    j=lax.bitwise_xor(block, me)
    return 2*turn(j//2, me%2)+j%2

def tn(a,b,ca,cb): return lax.dot_general(a,b,(((ca,),(cb,)),((),())),preferred_element_type=f32)

def fold8(a): return jnp.sum(a.reshape(a.shape[0]//8,8,a.shape[1]),axis=0)
def foldmax8(a): return jnp.max(a.reshape(a.shape[0]//8,8,a.shape[1]),axis=0)

def causal(s, fill):
    r=lax.broadcasted_iota(jnp.int32,s.shape,0); c=lax.broadcasted_iota(jnp.int32,s.shape,1)
    return jnp.where(r<=c,s,fill)

def fwd_kernel(me_ref,q_ref,k_ref,v_ref,_,ctx_ref,lse_ref,kt,sc,acc):
    i=pl.program_id(0)
    @pl.when(i==0)
    def _(): kt[...]=k_ref[0].T
    q=q_ref[0]
    def rows(j): return pl.ds(pl.multiple_of(j*BQ,BQ),BQ)
    def p1(j,m):
        s=jnp.dot(kt[rows(j),:],q,preferred_element_type=f32)
        sc[rows(j),:]=s
        return jnp.maximum(m,foldmax8(s))
    m=lax.fori_loop(0,i,p1,jnp.full((8,BQ),-1e30,f32))
    s=causal(jnp.dot(kt[rows(i),:],q,preferred_element_type=f32),-1e30)
    sc[rows(i),:]=s
    m=jnp.max(jnp.maximum(m,foldmax8(s)),axis=0,keepdims=True)*C2
    def p2(j,l):
        e=jnp.exp2(sc[rows(j),:]*C2-m)
        sc[rows(j),:]=e
        return l+fold8(e)
    l=jnp.sum(lax.fori_loop(0,i+1,p2,jnp.zeros((8,BQ),f32)),axis=0,keepdims=True)
    inv=1.0/l
    lse_ref[0]=m+jnp.log2(l)
    acc[...]=jnp.zeros_like(acc)
    def p3(j,_):
        p=(sc[rows(j),:]*inv).astype(bf16)
        acc[...]+=jnp.dot(v_ref[0,:,rows(j)],p,preferred_element_type=f32)
        return 0
    lax.fori_loop(0,i+1,p3,0)
    for a in range(BQ//BLK):
        pos=rel_pos(i*(BQ//BLK)+a,me_ref[0])
        ctx_ref[0,:,pl.ds(pl.multiple_of(pos*BLK,BLK),BLK)]=acc[:,a*BLK:(a+1)*BLK].astype(bf16)

def bwd_kernel(me_ref,q_ref,k_ref,v_ref,g_ref,lse_ref,_,out_ref,kt,vt,psc,dsc,g_sc,dq,dk,dv):
    i=pl.program_id(0)
    @pl.when(i==0)
    def _():
        kt[...]=k_ref[0].T
        vt[...]=v_ref[0].T
        dk[...]=jnp.zeros_like(dk); dv[...]=jnp.zeros_like(dv)
    def rows(j): return pl.ds(pl.multiple_of(j*BQ,BQ),BQ)
    for a in range(BQ//BLK):
        pos=rel_pos(i*(BQ//BLK)+a,me_ref[0])
        g_sc[:,a*BLK:(a+1)*BLK]=g_ref[0,:,pl.ds(pl.multiple_of(pos*BLK,BLK),BLK)]
    q=q_ref[0]; g=g_sc[...]; lse=lse_ref[0]
    def tile(j,d,diag):
        s=jnp.dot(kt[rows(j),:],q,preferred_element_type=f32)
        p=jnp.exp2(s*C2-lse)
        if diag: p=causal(p,0.0)
        dp=jnp.dot(vt[rows(j),:],g,preferred_element_type=f32)
        psc[rows(j),:]=p; dsc[rows(j),:]=dp
        return d+fold8(p*dp)
    d=lax.fori_loop(0,i,lambda j,d: tile(j,d,False),jnp.zeros((8,BQ),f32))
    delta=jnp.sum(tile(i,d,True),axis=0,keepdims=True)
    dq[...]=jnp.zeros_like(dq)
    def p2(j,_):
        p=psc[rows(j),:]
        ds=(p*(dsc[rows(j),:]-delta)*C).astype(bf16)
        dq[...]+=jnp.dot(k_ref[0,:,rows(j)],ds,preferred_element_type=f32)
        dk[:,rows(j)]+=tn(q,ds,1,1)
        dv[:,rows(j)]+=tn(g,p.astype(bf16),1,1)
        return 0
    lax.fori_loop(0,i+1,p2,0)
    for a in range(BQ//BLK):
        pos=rel_pos(i*(BQ//BLK)+a,me_ref[0])
        out_ref[0,0,:,pl.ds(pl.multiple_of(pos*BLK,BLK),BLK)]=dq[:,a*BLK:(a+1)*BLK].astype(bf16)
    @pl.when(i==NQ-1)
    def _():
        for b in range(T//BLK):
            at=pl.ds(pl.multiple_of(rel_pos(b,me_ref[0])*BLK,BLK),BLK)
            out_ref[1,0,:,at]=dk[:,b*BLK:(b+1)*BLK].astype(bf16)
            out_ref[2,0,:,at]=dv[:,b*BLK:(b+1)*BLK].astype(bf16)

NEL=(NQ*(NQ+1)//2)*BQ*BQ
def attn_call(kernel, ins, in_specs, out_specs, out_shape, scratch, flops, prev):
    al={}
    if prev is None: prev=ins[0]
    else: al={len(ins):0}
    return pl.pallas_call(kernel,
        grid_spec=pltpu.PrefetchScalarGridSpec(num_scalar_prefetch=1,grid=(NQ,),
            in_specs=in_specs+[pl.BlockSpec(memory_space=pl.ANY if al else pltpu.SMEM)],out_specs=out_specs,scratch_shapes=scratch),
        out_shape=out_shape,input_output_aliases=al,
        compiler_params=pltpu.CompilerParams(dimension_semantics=("arbitrary",),vmem_limit_bytes=40<<20),
        cost_estimate=pl.CostEstimate(flops=flops,bytes_accessed=3<<20,transcendentals=NEL))(*ins,prev)
def head_specs(h):
    full=pl.BlockSpec((1,E,T),lambda i,me:(h,0,0))
    return full,pl.BlockSpec((1,E,BQ),lambda i,me:(h,0,i)),pl.BlockSpec((1,1,BQ),lambda i,me:(0,0,i))
def attn_fwd(h,me,q,k,v,prev):
    full,qblk,lblk=head_specs(h)
    return attn_call(fwd_kernel,(me,q,k,v),[qblk,full,full],[full,lblk],
        [jax.ShapeDtypeStruct((NH,E,T),bf16),jax.ShapeDtypeStruct((1,1,T),f32)],
        [pltpu.VMEM((T,E),bf16),pltpu.VMEM((T,BQ),f32),pltpu.VMEM((E,BQ),f32)],NEL*1024,prev)
def attn_bwd(h,me,q,k,v,g,lse,prev):
    full,qblk,lblk=head_specs(h)
    return attn_call(bwd_kernel,(me,q,k,v,g,lse),[qblk,full,full,full,lblk],
        pl.BlockSpec((3,1,E,T),lambda i,me:(0,h,0,0)),jax.ShapeDtypeStruct((3,NH,E,T),bf16),
        [pltpu.VMEM((T,E),bf16),pltpu.VMEM((T,E),bf16),pltpu.VMEM((T,BQ),f32),pltpu.VMEM((T,BQ),f32),
         pltpu.VMEM((E,BQ),bf16),pltpu.VMEM((E,BQ),f32),pltpu.VMEM((E,T),f32),pltpu.VMEM((E,T),f32)],NEL*2048,prev)

LN_EPS=1e-5
GELU_COEF=0.044715
GELU_SCALE=0.7978845608028654
D=2304
F=1152
ANY=pl.ANY

def send(a, pairs):
    return lax.ppermute(a, 'tp', pairs)
def partner(a): return send(a, [(i, i ^ 1) for i in range(8)])
def hop_a(a):
    return send(a, [(i, i ^ (2 if i % 2 == 0 else 4)) for i in range(8)])
def hop_b(a): return send(a, [(i, i ^ (4 if i % 2 == 0 else 2)) for i in range(8)])
def after(x, *deps): return lax.optimization_barrier((x,)+deps)[0]

def add2(a, b): return (a.astype(f32)+b.astype(f32)).astype(bf16)

def layer_norm_fwd(token_rows, norm_gain, norm_bias):
    rows_f32 = token_rows.astype(f32)
    centered = rows_f32 - jnp.mean(rows_f32, axis=-1, keepdims=True)
    inv_std = lax.rsqrt(jnp.mean(centered * centered, axis=-1, keepdims=True) + LN_EPS)
    return (centered * inv_std * norm_gain + norm_bias).astype(bf16)

def ln_bwd_kernel(own, ro, a_in, b_in, rows, skip, gain, out, vec):
    i=pl.program_id(0)
    dh=(own[...].astype(f32)+ro[...].astype(f32))+(a_in[...].astype(f32)+b_in[...].astype(f32))
    r=rows[...].astype(f32)
    cen=r-jnp.mean(r,axis=-1,keepdims=True)
    rstd=lax.rsqrt(jnp.mean(cen*cen,axis=-1,keepdims=True)+LN_EPS)
    hat=cen*rstd
    gh=dh*gain[...]
    cg=gh-jnp.mean(gh,axis=-1,keepdims=True)
    sk=skip[...].astype(f32)
    o=(sk+rstd*(cg-hat*jnp.mean(gh*hat,axis=-1,keepdims=True))).astype(bf16)
    out[...]=o
    @pl.when(i==0)
    def _(): vec[...]=jnp.zeros_like(vec)
    vec[0]+=fold8(dh*hat); vec[1]+=fold8(dh); vec[2]+=fold8(o.astype(f32)); vec[3]+=fold8(sk)

def ln_bwd(parts, rows, skip, gain):
    R=64
    blk=pl.BlockSpec((R,D),lambda i:(i,0))
    out,vec=pl.pallas_call(ln_bwd_kernel,grid=(256//R,),
        in_specs=[blk]*6+[pl.BlockSpec((1,D),lambda i:(0,0))],
        out_specs=[blk,pl.BlockSpec((4,8,D),lambda i:(0,0,0))],
        out_shape=[jax.ShapeDtypeStruct((256,D),bf16),jax.ShapeDtypeStruct((4,8,D),f32)],
        compiler_params=pltpu.CompilerParams(dimension_semantics=("arbitrary",)),
        cost_estimate=pl.CostEstimate(flops=256*D*1000,bytes_accessed=6<<20,transcendentals=0))(*parts,rows,skip,gain.reshape(1,D))
    return out,jnp.sum(vec,axis=1)

def call(kernel, grid, in_specs, out_specs, out_shape, scratch, flops, vmem, args):
    return pl.pallas_call(kernel,grid=grid,in_specs=in_specs,out_specs=out_specs,out_shape=out_shape,
        scratch_shapes=scratch,compiler_params=pltpu.CompilerParams(dimension_semantics=("arbitrary",)*len(grid),vmem_limit_bytes=vmem<<20),
        cost_estimate=pl.CostEstimate(flops=flops,bytes_accessed=30<<20,transcendentals=0))(*args)

SEM8=lambda: pltpu.SemaphoreType.DMA((8,))

def gelu_kernel(blk_ref, z, u, slope):
    zf=z[...].astype(f32)
    th=jnp.tanh(GELU_SCALE*(zf+GELU_COEF*zf*zf*zf))
    u[...]=(0.5*zf*(1.0+th)).astype(bf16)
    slope[...]=0.5*(1.0+th)+0.5*zf*(1.0-th*th)*GELU_SCALE*(1.0+3.0*GELU_COEF*zf*zf)

def gelu(blk, z):
    out=pl.BlockSpec((BLK,F),lambda p,blk:(p,0))
    return pl.pallas_call(gelu_kernel,name="gelu",
        grid_spec=pltpu.PrefetchScalarGridSpec(num_scalar_prefetch=1,grid=(8,),
            in_specs=[pl.BlockSpec((BLK,F),lambda p,blk:(blk[p],0))],out_specs=[out,out]),
        out_shape=[jax.ShapeDtypeStruct((T,F),bf16),jax.ShapeDtypeStruct((T,F),f32)],
        compiler_params=pltpu.CompilerParams(dimension_semantics=("arbitrary",)),
        cost_estimate=pl.CostEstimate(flops=T*F*1000,bytes_accessed=20<<20,transcendentals=T*F))(blk,z)

def mlp(first, pieces, slope, w2, w1, prev):
    n=len(pieces)//2
    def kernel(*refs):
        dy=refs[:2*n]; sl,w2h,w1h=refs[2*n:2*n+3]
        refs=refs[2*n+(3 if prev is None else 4):]
        dz_ref,db_ref=refs[:2]; dh=refs[2:2+2*n]
        x,w2s,w1s,st,xsem,wsem,osem=refs[2+2*n:]
        s=pl.program_id(0)
        def wcopy(k): return pltpu.make_async_copy((w2h,w1h)[k],(w2s,w1s)[k],wsem.at[k])
        def xcopy(p): return pltpu.make_async_copy(dy[p],x.at[p*BLK:(p+1)*BLK],xsem.at[p])
        def ocopy(p): return pltpu.make_async_copy(st.at[p*BLK:(p+1)*BLK],dh[p],osem.at[p])
        @pl.when(s==0)
        def _():
            wcopy(0).start()
            for p in range(2*n): xcopy(p).start()
            wcopy(1).start()
            db_ref[...]=jnp.zeros_like(db_ref)
            wcopy(0).wait()
        for k in range(n):
            @pl.when(s==k)
            def _():
                xcopy(2*k).wait(); xcopy(2*k+1).wait()
        rows=pl.ds(pl.multiple_of(s*2*BLK,2*BLK),2*BLK)
        dz=(tn(x[rows,:],w2s[...],1,1)*sl[...]).astype(bf16)
        dz_ref[...]=dz
        db_ref[...]+=fold8(dz.astype(f32))
        @pl.when(s==0)
        def _(): wcopy(1).wait()
        st[rows,:]=tn(dz_ref[...],w1s[...],1,1).astype(bf16)
        for k in range(n):
            @pl.when(s==k)
            def _():
                ocopy(2*k).start(); ocopy(2*k+1).start()
        @pl.when(s==n-1)
        def _():
            for p in range(2*n): ocopy(p).wait()
    any_=pl.BlockSpec(memory_space=ANY)
    step=pl.BlockSpec((2*BLK,F),lambda s:(s+first,0))
    outs=pl.pallas_call(kernel,grid=(n,),
        in_specs=[any_]*(2*n)+[step]+[any_]*(2 if prev is None else 3),
        out_specs=[step,pl.BlockSpec((8,F),lambda s:(0,0))]+[any_]*(2*n),
        out_shape=[jax.ShapeDtypeStruct((T,F),bf16),jax.ShapeDtypeStruct((8,F),f32)]+[jax.ShapeDtypeStruct((BLK,D),bf16)]*(2*n),
        scratch_shapes=[pltpu.VMEM((2*n*BLK,D),bf16),pltpu.VMEM((F,D),bf16),pltpu.VMEM((D,F),bf16),pltpu.VMEM((2*n*BLK,D),bf16),
         pltpu.SemaphoreType.DMA((2*n,)),pltpu.SemaphoreType.DMA((2,)),pltpu.SemaphoreType.DMA((2*n,))],
        input_output_aliases={} if prev is None else {2*n+3:0},
        compiler_params=pltpu.CompilerParams(dimension_semantics=("arbitrary",),vmem_limit_bytes=48<<20),
        cost_estimate=pl.CostEstimate(flops=n*T*D*F,bytes_accessed=20<<20,transcendentals=0))(*pieces,slope,w2,w1,*(() if prev is None else (prev,)))
    return outs[0],outs[1],list(outs[2:])

def attn_in_grad(chips, dqkv, wqkv):
    c0,c1=chips
    def kernel(g,w,*refs):
        dh=refs[:4]; st,sem=refs[4:]
        s=pl.program_id(0)
        def ocopy(p): return pltpu.make_async_copy(st.at[p*BLK:(p+1)*BLK],dh[p],sem.at[p])
        rows=pl.ds(pl.multiple_of(s*2*BLK,2*BLK),2*BLK)
        st[rows,:]=tn(g[...],w[...],0,0).astype(bf16)
        for k in range(2):
            @pl.when(s==k)
            def _():
                ocopy(2*k).start(); ocopy(2*k+1).start()
        @pl.when(s==1)
        def _():
            for p in range(4): ocopy(p).wait()
    K=3*NH*E
    return call(kernel,(2,),[pl.BlockSpec((K,2*BLK),lambda s:(0,c0+(c1-c0)*s)),pl.BlockSpec((K,D),lambda s:(0,0))],
        [pl.BlockSpec(memory_space=ANY)]*4,[jax.ShapeDtypeStruct((BLK,D),bf16)]*4,
        [pltpu.VMEM((4*BLK,D),bf16),pltpu.SemaphoreType.DMA((4,))],T*D*K,40,(dqkv,wqkv))

def gathered_mm(body, pieces, other, other_spec, grid, out_spec, out_shape, flops, vmem=50, cols=(0,D), into=None):
    def kernel(*refs):
        ps=refs[:8]; o_ref=refs[8]; out,full,sem=refs[-3:]
        @pl.when(pl.program_id(0)==0)
        def _():
            cs=[pltpu.make_async_copy(ps[p].at[:,cols[0]:cols[1]],full.at[p*BLK:(p+1)*BLK],sem.at[p]) for p in range(8)]
            for c in cs: c.start()
            for c in cs: c.wait()
        out[...]=body(full,o_ref,pl.program_id(0)).astype(out.dtype)
    any_=pl.BlockSpec(memory_space=ANY)
    extra=() if into is None else (into,)
    return pl.pallas_call(kernel,grid=grid,in_specs=[any_]*8+[other_spec]+[any_]*len(extra),out_specs=out_spec,out_shape=out_shape,
        scratch_shapes=[pltpu.VMEM((T,cols[1]-cols[0]),bf16),SEM8()],input_output_aliases={9:0} if extra else {},
        compiler_params=pltpu.CompilerParams(dimension_semantics=("arbitrary",)*len(grid),vmem_limit_bytes=vmem<<20),
        cost_estimate=pl.CostEstimate(flops=flops,bytes_accessed=30<<20,transcendentals=0))(*pieces,other,*extra)

def solution(mesh):
    def layer(x_in, x_mid, d_out, q_saved, k_saved, v_saved, z_saved, g1, b1, g2, b2, w_qkv, w_proj, w_fc1, w_fc2):
        me=lax.axis_index('tp').astype(jnp.int32)
        me1=jnp.reshape(me,(1,))
        p8=jnp.arange(8,dtype=jnp.int32)
        blk=lax.bitwise_xor(me,2*turn(p8//2,me%2)+p8%2)
        x_in, x_mid, d_out, z = x_in[0], x_mid[0], d_out[0], z_saved[0]
        heads=lambda a: a[0].transpose(1,2,0)
        q,k,v=heads(q_saved),heads(k_saved),heads(v_saved)
        wqkv=w_qkv.transpose(0,2,3,1).reshape(3*NH*E,D)
        wo=w_proj.reshape(NH*E,D)
        dya,dyb,dyp=hop_a(d_out),hop_b(d_out),partner(d_out)
        u,slope=gelu(blk,z)
        dz,db_0,(o0,o1)=mlp(0,[d_out,dyp],slope,w_fc2,w_fc1,None)
        dya=after(dya,db_0)
        dyd=hop_b(dya)
        h2_local=layer_norm_fwd(after(x_mid,dya),g2,b2)
        h2a,h2b,h2p=hop_a(h2_local),hop_b(h2_local),partner(h2_local)
        dypa,dypb=partner(dya),partner(dyb)
        dz,db_1,(pa0,pa1,pb0,pb1)=mlp(1,[dya,dypb,dyb,dypa],slope,w_fc2,w_fc1,dz)
        ra,rb,ro=partner(pb1),partner(pa1),partner(o1)
        a_in=hop_a(add2(pa0,ra))
        dypd=partner(dyd)
        dz,db_2,(pd0,pd1)=mlp(3,[dyd,dypd],slope,w_fc2,w_fc1,dz)
        d_sum=add2(pd0,partner(pd1))
        d_in=hop_a(d_sum)
        ctx,lse0=attn_fwd(0,me1,after(q,d_sum),k,v,None)
        ctx,lse1=attn_fwd(1,me1,q,k,v,ctx)
        b_sum=(pb0.astype(f32)+after(rb,lse1).astype(f32)+d_in.astype(f32)).astype(bf16)
        b_in=hop_b(b_sum)
        h2a=after(h2a,b_sum)
        h2d=hop_b(h2a); h2pa,h2pb=partner(h2a),partner(h2b)
        ctx,lse2=attn_fwd(2,me1,after(q,b_sum),k,v,ctx)
        mid,vec2=ln_bwd((after(o0,lse2),ro,a_in,b_in),x_mid,d_out,g2)
        grad_bfc1=jnp.sum(db_0+db_1+db_2,axis=0)
        dxa,dxb,dxp=hop_a(mid),hop_b(mid),partner(mid)
        dys=[d_out,dyp,dya,dypb,dyb,dypa,dyd,dypd]
        grad_wfc2=gathered_mm(lambda full,o,s: tn(o[...],full[...],0,0),dys,after(u,mid),pl.BlockSpec((T,384),lambda s:(0,s)),(3,),
            pl.BlockSpec((384,D),lambda s:(s,0)),jax.ShapeDtypeStruct((F,D),f32),2*T*D*F)
        h1_local=layer_norm_fwd(after(x_in,mid),g1,b1)
        dxa=after(dxa,grad_wfc2,h1_local)
        dxd=hop_b(dxa)
        h1_local=after(h1_local,dxa)
        h1a,h1b,h1p=hop_a(h1_local),hop_b(h1_local),partner(h1_local)
        dxpa,dxpb=partner(dxa),partner(dxb)
        h2pd=partner(after(h2d,grad_wfc2))
        h2=[h2_local,h2p,h2a,h2pb,h2b,h2pa,h2d,h2pd]
        def w1_half(k,r,into):
            return gathered_mm(lambda full,o,s: tn(full[:,pl.ds(pl.multiple_of(s*384,384),384)],o[...],0,0),h2,r,pl.BlockSpec((T,F),lambda s:(0,0)),(3,),
                pl.BlockSpec((384,F),lambda s:(s+3*k,0)),jax.ShapeDtypeStruct((D,F),f32),T*D*F,cols=(F*k,F*(k+1)),into=into)
        grad_wfc1=w1_half(0,after(dz,dxa),None)
        dxpd=partner(dxd)
        dx1=[mid,dxp,dxa,dxpb,dxb,dxpa,dxd,dxpd]
        dctx=gathered_mm(lambda full,o,s: tn(o[...],full[pl.ds(pl.multiple_of(s*512,512),512),:],1,1),dx1,after(wo,grad_wfc1),pl.BlockSpec((NH*E,D),lambda s:(0,0)),(4,),
            pl.BlockSpec((NH*E,512),lambda s:(0,s)),jax.ShapeDtypeStruct((NH*E,T),bf16),2*T*D*NH*E).reshape(NH,E,T)
        dqkv=attn_bwd(0,me1,q,k,v,dctx,lse0,None)
        dqkv=attn_bwd(1,me1,q,k,v,dctx,lse1,dqkv)
        h1a=after(h1a,dqkv)
        h1d=hop_b(h1a); h1pa,h1pb=partner(h1a),partner(h1b)
        dqkv=attn_bwd(2,me1,q,k,v,dctx,lse2,dqkv)
        dqkv=dqkv.reshape(3*NH*E,T)
        pd0,pd1,pa0,pa1=attn_in_grad((3,1),dqkv,wqkv)
        d_sum=add2(pd0,partner(pd1))
        d_in=hop_a(d_sum)
        rb=partner(pa1)
        pb0,pb1,o0,o1=attn_in_grad((2,0),after(dqkv,d_sum),wqkv)
        ra,ro=partner(pb1),partner(o1)
        a_sum=add2(pa0,ra)
        a_in=hop_a(a_sum)
        grad_wproj=gathered_mm(lambda full,o,s: jnp.dot(o[...],full[:,pl.ds(pl.multiple_of(s*768,768),768)],preferred_element_type=f32),dx1,after(ctx,a_sum).reshape(NH*E,T),pl.BlockSpec((NH*E,T),lambda s:(0,0)),(3,),
            pl.BlockSpec((NH*E,768),lambda s:(0,s)),jax.ShapeDtypeStruct((NH*E,D),f32),2*T*D*NH*E)
        b_sum=(pb0.astype(f32)+after(rb,grad_wproj).astype(f32)+d_in.astype(f32)).astype(bf16)
        b_in=hop_b(b_sum)
        h1pd=partner(after(h1d,dqkv))
        h1=[h1_local,h1p,h1a,h1pb,h1b,h1pa,h1d,h1pd]
        grad_wqkv=gathered_mm(lambda full,o,s: jnp.dot(o[...],full[...],preferred_element_type=f32),h1,after(dqkv,b_sum),pl.BlockSpec((288,T),lambda s:(s,0)),(3,),
            pl.BlockSpec((288,D),lambda s:(s,0)),jax.ShapeDtypeStruct((3*NH*E,D),f32),6*T*D*NH*E)
        grad_bqkv=jnp.sum(dqkv,axis=1,dtype=f32).reshape(3,NH,E)
        dx,vec1=ln_bwd((after(o0,grad_wqkv),ro,a_in,b_in),x_in,mid,g1)
        grad_vecs=jnp.concatenate([vec1[:2],vec2],axis=0)
        grad_wfc1=w1_half(1,after(dz,dx),grad_wfc1)
        for k in (1,2,4):
            grad_vecs=grad_vecs+send(grad_vecs,[(i,i^k) for i in range(8)])
        grad_wproj=grad_wproj.reshape(NH,E,D)
        grad_wqkv=grad_wqkv.reshape(3,NH,E,D).transpose(0,3,1,2)
        return dx[None], grad_wqkv, grad_bqkv, grad_wproj, grad_wfc1, grad_bfc1, grad_wfc2, grad_vecs

    tok_spec = P('dp', 'tp', None)
    head_spec = P('dp', None, 'tp', None)
    in_specs = (tok_spec, tok_spec, tok_spec, head_spec, head_spec, head_spec, P('dp', None, 'tp'),
                P(None), P(None), P(None), P(None),
                P(None, None, 'tp', None), P('tp', None, None), P(None, 'tp'), P('tp', None))
    out_specs = (tok_spec, P('dp', None, 'tp', None), P('dp', 'tp', None), P(('dp', 'tp'), None, None),
                 P('dp', 'tp'), P(('dp', 'tp')), P(('dp', 'tp'), None), P('dp', None))
    return jax.shard_map(layer, mesh=mesh, in_specs=in_specs, out_specs=out_specs, check_vma=False)
```

```python
import jax, jax.numpy as jnp
from jax import lax
from jax.experimental import pallas as pl
from jax.experimental.pallas import tpu as pltpu
from jax.sharding import PartitionSpec as P
T=2048; E=96; NH=3; BQ=512; NQ=T//BQ; BLK=256
C=E**-0.5; C2=C*1.4426950408889634
f32=jnp.float32; bf16=jnp.bfloat16

def turn(h, core):
    return jnp.where(core==0, h, (h%2)*2+h//2)

def rel_pos(block, me):
    j=lax.bitwise_xor(block, me)
    return 2*turn(j//2, me%2)+j%2

def tn(a,b,ca,cb): return lax.dot_general(a,b,(((ca,),(cb,)),((),())),preferred_element_type=f32)

def fold8(a): return jnp.sum(a.reshape(a.shape[0]//8,8,a.shape[1]),axis=0)
def foldmax8(a): return jnp.max(a.reshape(a.shape[0]//8,8,a.shape[1]),axis=0)

def causal(s, fill):
    r=lax.broadcasted_iota(jnp.int32,s.shape,0); c=lax.broadcasted_iota(jnp.int32,s.shape,1)
    return jnp.where(r<=c,s,fill)

def fwd_kernel(me_ref,q_ref,k_ref,v_ref,_,ctx_ref,lse_ref,kt,sc,acc):
    i=pl.program_id(1)
    @pl.when(i==0)
    def _(): kt[...]=k_ref[0].T
    q=q_ref[0]
    def rows(j): return pl.ds(pl.multiple_of(j*BQ,BQ),BQ)
    def p1(j,m):
        s=jnp.dot(kt[rows(j),:],q,preferred_element_type=f32)
        sc[rows(j),:]=s
        return jnp.maximum(m,foldmax8(s))
    m=lax.fori_loop(0,i,p1,jnp.full((8,BQ),-1e30,f32))
    s=causal(jnp.dot(kt[rows(i),:],q,preferred_element_type=f32),-1e30)
    sc[rows(i),:]=s
    m=jnp.max(jnp.maximum(m,foldmax8(s)),axis=0,keepdims=True)*C2
    def p2(j,l):
        e=jnp.exp2(sc[rows(j),:]*C2-m)
        sc[rows(j),:]=e
        return l+fold8(e)
    l=jnp.sum(lax.fori_loop(0,i+1,p2,jnp.zeros((8,BQ),f32)),axis=0,keepdims=True)
    inv=1.0/l
    lse_ref[0]=m+jnp.log2(l)
    acc[...]=jnp.zeros_like(acc)
    def p3(j,_):
        p=(sc[rows(j),:]*inv).astype(bf16)
        acc[...]+=jnp.dot(v_ref[0,:,rows(j)],p,preferred_element_type=f32)
        return 0
    lax.fori_loop(0,i+1,p3,0)
    for a in range(BQ//BLK):
        pos=rel_pos(i*(BQ//BLK)+a,me_ref[0])
        ctx_ref[0,:,pl.ds(pl.multiple_of(pos*BLK,BLK),BLK)]=acc[:,a*BLK:(a+1)*BLK].astype(bf16)

def bwd_kernel(me_ref,q_ref,k_ref,v_ref,g_ref,lse_ref,_,out_ref,kt,vt,psc,dsc,g_sc,dq,dk,dv):
    i=pl.program_id(1)
    @pl.when(i==0)
    def _():
        kt[...]=k_ref[0].T
        vt[...]=v_ref[0].T
        dk[...]=jnp.zeros_like(dk); dv[...]=jnp.zeros_like(dv)
    def rows(j): return pl.ds(pl.multiple_of(j*BQ,BQ),BQ)
    for a in range(BQ//BLK):
        pos=rel_pos(i*(BQ//BLK)+a,me_ref[0])
        g_sc[:,a*BLK:(a+1)*BLK]=g_ref[0,:,pl.ds(pl.multiple_of(pos*BLK,BLK),BLK)]
    q=q_ref[0]; g=g_sc[...]; lse=lse_ref[0]
    def tile(j,d,diag):
        s=jnp.dot(kt[rows(j),:],q,preferred_element_type=f32)
        p=jnp.exp2(s*C2-lse)
        if diag: p=causal(p,0.0)
        dp=jnp.dot(vt[rows(j),:],g,preferred_element_type=f32)
        psc[rows(j),:]=p; dsc[rows(j),:]=dp
        return d+fold8(p*dp)
    d=lax.fori_loop(0,i,lambda j,d: tile(j,d,False),jnp.zeros((8,BQ),f32))
    delta=jnp.sum(tile(i,d,True),axis=0,keepdims=True)
    dq[...]=jnp.zeros_like(dq)
    def p2(j,_):
        p=psc[rows(j),:]
        ds=(p*(dsc[rows(j),:]-delta)*C).astype(bf16)
        dq[...]+=jnp.dot(k_ref[0,:,rows(j)],ds,preferred_element_type=f32)
        dk[:,rows(j)]+=tn(q,ds,1,1)
        dv[:,rows(j)]+=tn(g,p.astype(bf16),1,1)
        return 0
    lax.fori_loop(0,i+1,p2,0)
    for a in range(BQ//BLK):
        pos=rel_pos(i*(BQ//BLK)+a,me_ref[0])
        out_ref[0,0,:,pl.ds(pl.multiple_of(pos*BLK,BLK),BLK)]=dq[:,a*BLK:(a+1)*BLK].astype(bf16)
    @pl.when(i==NQ-1)
    def _():
        for b in range(T//BLK):
            at=pl.ds(pl.multiple_of(rel_pos(b,me_ref[0])*BLK,BLK),BLK)
            out_ref[1,0,:,at]=dk[:,b*BLK:(b+1)*BLK].astype(bf16)
            out_ref[2,0,:,at]=dv[:,b*BLK:(b+1)*BLK].astype(bf16)

NEL=(NQ*(NQ+1)//2)*BQ*BQ
def attn_call(kernel, n, ins, in_specs, out_specs, out_shape, scratch, flops, prev):
    al={}
    if prev is None: prev=ins[0]
    else: al={len(ins):0}
    return pl.pallas_call(kernel,
        grid_spec=pltpu.PrefetchScalarGridSpec(num_scalar_prefetch=1,grid=(n,NQ),
            in_specs=in_specs+[pl.BlockSpec(memory_space=pl.ANY if al else pltpu.SMEM)],out_specs=out_specs,scratch_shapes=scratch),
        out_shape=out_shape,input_output_aliases=al,
        compiler_params=pltpu.CompilerParams(dimension_semantics=("arbitrary","arbitrary"),vmem_limit_bytes=40<<20),
        cost_estimate=pl.CostEstimate(flops=n*flops,bytes_accessed=n*(3<<20),transcendentals=n*NEL))(*ins,prev)
def head_specs(h0):
    full=pl.BlockSpec((1,E,T),lambda h,i,me:(h+h0,0,0))
    return full,pl.BlockSpec((1,E,BQ),lambda h,i,me:(h+h0,0,i)),pl.BlockSpec((1,1,BQ),lambda h,i,me:(h,0,i))
def attn_fwd(h0,n,me,q,k,v,prev):
    full,qblk,lblk=head_specs(h0)
    return attn_call(fwd_kernel,n,(me,q,k,v),[qblk,full,full],[full,lblk],
        [jax.ShapeDtypeStruct((NH,E,T),bf16),jax.ShapeDtypeStruct((n,1,T),f32)],
        [pltpu.VMEM((T,E),bf16),pltpu.VMEM((T,BQ),f32),pltpu.VMEM((E,BQ),f32)],NEL*1024,prev)
def attn_bwd(h0,n,me,q,k,v,g,lse,prev):
    full,qblk,lblk=head_specs(h0)
    return attn_call(bwd_kernel,n,(me,q,k,v,g,lse),[qblk,full,full,full,lblk],
        pl.BlockSpec((3,1,E,T),lambda h,i,me:(0,h+h0,0,0)),jax.ShapeDtypeStruct((3,NH,E,T),bf16),
        [pltpu.VMEM((T,E),bf16),pltpu.VMEM((T,E),bf16),pltpu.VMEM((T,BQ),f32),pltpu.VMEM((T,BQ),f32),
         pltpu.VMEM((E,BQ),bf16),pltpu.VMEM((E,BQ),f32),pltpu.VMEM((E,T),f32),pltpu.VMEM((E,T),f32)],NEL*2048,prev)

LN_EPS=1e-5
GELU_COEF=0.044715
GELU_SCALE=0.7978845608028654
D=2304
F=1152
ANY=pl.ANY

def send(a, pairs):
    return lax.ppermute(a, 'tp', pairs)
def partner(a): return send(a, [(i, i ^ 1) for i in range(8)])
def hop_a(a):
    return send(a, [(i, i ^ (2 if i % 2 == 0 else 4)) for i in range(8)])
def hop_b(a): return send(a, [(i, i ^ (4 if i % 2 == 0 else 2)) for i in range(8)])
def after(x, *deps): return lax.optimization_barrier((x,)+deps)[0]

def add2(a, b): return (a.astype(f32)+b.astype(f32)).astype(bf16)

def layer_norm_fwd(token_rows, norm_gain, norm_bias):
    rows_f32 = token_rows.astype(f32)
    centered = rows_f32 - jnp.mean(rows_f32, axis=-1, keepdims=True)
    inv_std = lax.rsqrt(jnp.mean(centered * centered, axis=-1, keepdims=True) + LN_EPS)
    return (centered * inv_std * norm_gain + norm_bias).astype(bf16)

def ln_bwd_kernel(own, ro, a_in, b_in, rows, skip, gain, out, vec):
    i=pl.program_id(0)
    dh=(own[...].astype(f32)+ro[...].astype(f32))+(a_in[...].astype(f32)+b_in[...].astype(f32))
    r=rows[...].astype(f32)
    cen=r-jnp.mean(r,axis=-1,keepdims=True)
    rstd=lax.rsqrt(jnp.mean(cen*cen,axis=-1,keepdims=True)+LN_EPS)
    hat=cen*rstd
    gh=dh*gain[...]
    cg=gh-jnp.mean(gh,axis=-1,keepdims=True)
    sk=skip[...].astype(f32)
    o=(sk+rstd*(cg-hat*jnp.mean(gh*hat,axis=-1,keepdims=True))).astype(bf16)
    out[...]=o
    @pl.when(i==0)
    def _(): vec[...]=jnp.zeros_like(vec)
    vec[0]+=fold8(dh*hat); vec[1]+=fold8(dh); vec[2]+=fold8(o.astype(f32)); vec[3]+=fold8(sk)

def ln_bwd(parts, rows, skip, gain):
    R=64
    blk=pl.BlockSpec((R,D),lambda i:(i,0))
    out,vec=pl.pallas_call(ln_bwd_kernel,grid=(256//R,),
        in_specs=[blk]*6+[pl.BlockSpec((1,D),lambda i:(0,0))],
        out_specs=[blk,pl.BlockSpec((4,8,D),lambda i:(0,0,0))],
        out_shape=[jax.ShapeDtypeStruct((256,D),bf16),jax.ShapeDtypeStruct((4,8,D),f32)],
        compiler_params=pltpu.CompilerParams(dimension_semantics=("arbitrary",)),
        cost_estimate=pl.CostEstimate(flops=256*D*1000,bytes_accessed=6<<20,transcendentals=0))(*parts,rows,skip,gain.reshape(1,D))
    return out,jnp.sum(vec,axis=1)

def call(kernel, grid, in_specs, out_specs, out_shape, scratch, flops, args):
    return pl.pallas_call(kernel,grid=grid,in_specs=in_specs,out_specs=out_specs,out_shape=out_shape,
        scratch_shapes=scratch,compiler_params=pltpu.CompilerParams(dimension_semantics=("arbitrary",)*len(grid),vmem_limit_bytes=40<<20),
        cost_estimate=pl.CostEstimate(flops=flops,bytes_accessed=30<<20,transcendentals=0))(*args)

def gelu_kernel(blk_ref, z, u, slope):
    zf=z[...].astype(f32)
    th=jnp.tanh(GELU_SCALE*(zf+GELU_COEF*zf*zf*zf))
    u[...]=(0.5*zf*(1.0+th)).astype(bf16)
    slope[...]=0.5*(1.0+th)+0.5*zf*(1.0-th*th)*GELU_SCALE*(1.0+3.0*GELU_COEF*zf*zf)

def gelu(blk, z):
    out=pl.BlockSpec((BLK,F),lambda p,blk:(p,0))
    return pl.pallas_call(gelu_kernel,name="gelu",
        grid_spec=pltpu.PrefetchScalarGridSpec(num_scalar_prefetch=1,grid=(8,),
            in_specs=[pl.BlockSpec((BLK,F),lambda p,blk:(blk[p],0))],out_specs=[out,out]),
        out_shape=[jax.ShapeDtypeStruct((T,F),bf16),jax.ShapeDtypeStruct((T,F),f32)],
        compiler_params=pltpu.CompilerParams(dimension_semantics=("arbitrary",)),
        cost_estimate=pl.CostEstimate(flops=T*F*1000,bytes_accessed=20<<20,transcendentals=T*F))(blk,z)

def mlp(first, pieces, slope, w2, w1, prev):
    n=len(pieces)//2
    def kernel(*refs):
        dy=refs[:2*n]; sl,w2h,w1h=refs[2*n:2*n+3]
        refs=refs[2*n+(3 if prev is None else 4):]
        dz_ref,db_ref=refs[:2]; dh=refs[2:2+2*n]
        x,w2s,w1s,st,xsem,wsem,osem=refs[2+2*n:]
        s=pl.program_id(0)
        class wcopy:
            def __init__(self, k):
                h,v=((w2h,w2s),(w1h,w1s))[k]
                r=v.shape[0]//4
                self.cs=[pltpu.make_async_copy(h.at[j*r:(j+1)*r],v.at[j*r:(j+1)*r],wsem.at[k,j]) for j in range(4)]
            def start(self):
                for c in self.cs: c.start()
            def wait(self):
                for c in self.cs: c.wait()
        def xcopy(p): return pltpu.make_async_copy(dy[p],x.at[p*BLK:(p+1)*BLK],xsem.at[p])
        def ocopy(p): return pltpu.make_async_copy(st.at[p*BLK:(p+1)*BLK],dh[p],osem.at[p])
        @pl.when(s==0)
        def _():
            xcopy(0).start()
            wcopy(0).start()
            for p in range(1,2*n): xcopy(p).start()
            wcopy(1).start()
            db_ref[...]=jnp.zeros_like(db_ref)
            wcopy(0).wait()
        for k in range(2*n):
            @pl.when(s==k)
            def _(): xcopy(k).wait()
        rows=pl.ds(pl.multiple_of(s*BLK,BLK),BLK)
        dz=(tn(x[rows,:],w2s[...],1,1)*sl[...]).astype(bf16)
        dz_ref[...]=dz
        db_ref[...]+=fold8(dz.astype(f32))
        @pl.when(s==0)
        def _(): wcopy(1).wait()
        def part(c,_):
            at=pl.ds(pl.multiple_of(c*768,768),768)
            st[rows,at]=tn(dz_ref[...],w1s[at,:],1,1).astype(bf16)
            return 0
        lax.fori_loop(0,3,part,0)
        for k in range(2*n):
            @pl.when(s==k)
            def _(): ocopy(k).start()
        @pl.when(s==2*n-1)
        def _():
            for p in range(2*n): ocopy(p).wait()
    any_=pl.BlockSpec(memory_space=ANY)
    step=pl.BlockSpec((BLK,F),lambda s:(s+2*first,0))
    outs=pl.pallas_call(kernel,grid=(2*n,),
        in_specs=[any_]*(2*n)+[step]+[any_]*(2 if prev is None else 3),
        out_specs=[step,pl.BlockSpec((8,F),lambda s:(0,0))]+[any_]*(2*n),
        out_shape=[jax.ShapeDtypeStruct((T,F),bf16),jax.ShapeDtypeStruct((8,F),f32)]+[jax.ShapeDtypeStruct((BLK,D),bf16)]*(2*n),
        scratch_shapes=[pltpu.VMEM((2*n*BLK,D),bf16),pltpu.VMEM((F,D),bf16),pltpu.VMEM((D,F),bf16),pltpu.VMEM((2*n*BLK,D),bf16),
         pltpu.SemaphoreType.DMA((2*n,)),pltpu.SemaphoreType.DMA((2,4)),pltpu.SemaphoreType.DMA((2*n,))],
        input_output_aliases={} if prev is None else {2*n+3:0},
        compiler_params=pltpu.CompilerParams(dimension_semantics=("arbitrary",),vmem_limit_bytes=48<<20),
        cost_estimate=pl.CostEstimate(flops=n*T*D*F,bytes_accessed=20<<20,transcendentals=0))(*pieces,slope,w2,w1,*(() if prev is None else (prev,)))
    return outs[0],outs[1],list(outs[2:])

def attn_in_grad(chips, dqkv, wqkv):
    c0,c1=chips
    def kernel(g,w,*refs):
        dh=refs[:4]; st,sem=refs[4:]
        s=pl.program_id(0)
        def ocopy(p): return pltpu.make_async_copy(st.at[p*BLK:(p+1)*BLK],dh[p],sem.at[p])
        rows=pl.ds(pl.multiple_of(s*BLK,BLK),BLK)
        def part(c,_):
            at=pl.ds(pl.multiple_of(c*768,768),768)
            st[rows,at]=tn(g[...],w[:,at],0,0).astype(bf16)
            return 0
        lax.fori_loop(0,3,part,0)
        for k in range(4):
            @pl.when(s==k)
            def _(): ocopy(k).start()
        @pl.when(s==3)
        def _():
            for p in range(4): ocopy(p).wait()
    K=3*NH*E
    return call(kernel,(4,),[pl.BlockSpec((K,BLK),lambda s:(0,2*(c0+(c1-c0)*(s//2))+s%2)),pl.BlockSpec((K,D),lambda s:(0,0))],
        [pl.BlockSpec(memory_space=ANY)]*4,[jax.ShapeDtypeStruct((BLK,D),bf16)]*4,
        [pltpu.VMEM((4*BLK,D),bf16),pltpu.SemaphoreType.DMA((4,))],T*D*K,(dqkv,wqkv))

def gathered_mm(body, pieces, other, n, out_spec, out_shape, flops, cols=(0,D), into=None):
    W=(cols[1]-cols[0])//n
    def kernel(*refs):
        ps=refs[:8]; o_ref=refs[8]; out,full,sem=refs[-3:]
        s=pl.program_id(0)
        def copy(t,p): return pltpu.make_async_copy(ps[p].at[:,cols[0]+t*W:cols[0]+(t+1)*W],full.at[t,p*BLK:(p+1)*BLK],sem.at[t,p])
        @pl.when(s==0)
        def _():
            for t in range(n):
                for p in range(8): copy(t,p).start()
        for t in range(n):
            @pl.when(s==t)
            def _():
                for p in range(8): copy(t,p).wait()
        out[...]=body(full[s],o_ref)
    any_=pl.BlockSpec(memory_space=ANY)
    extra=() if into is None else (into,)
    return pl.pallas_call(kernel,grid=(n,),in_specs=[any_]*8+[pl.BlockSpec(other.shape,lambda s:(0,0))]+[any_]*len(extra),out_specs=out_spec,out_shape=out_shape,
        scratch_shapes=[pltpu.VMEM((n,T,W),bf16),pltpu.SemaphoreType.DMA((n,8))],input_output_aliases={9:0} if extra else {},
        compiler_params=pltpu.CompilerParams(dimension_semantics=("arbitrary",),vmem_limit_bytes=60<<20),
        cost_estimate=pl.CostEstimate(flops=flops,bytes_accessed=30<<20,transcendentals=0))(*pieces,other,*extra)

def ctx_grad(first, pieces, wo, into):
    n=len(pieces)//2
    def kernel(*refs):
        ps=refs[:2*n]; w=refs[2*n]; out,full,sem=refs[-3:]
        s=pl.program_id(0)
        def copy(p): return pltpu.make_async_copy(ps[p],full.at[p//2,(p%2)*BLK:(p%2+1)*BLK],sem.at[p])
        @pl.when(s==0)
        def _():
            for p in range(2*n): copy(p).start()
        for k in range(n):
            @pl.when(s==k)
            def _():
                copy(2*k).wait(); copy(2*k+1).wait()
        out[...]=tn(w[...],full[s],1,1).astype(bf16)
    any_=pl.BlockSpec(memory_space=ANY)
    extra=() if into is None else (into,)
    return pl.pallas_call(kernel,grid=(n,),in_specs=[any_]*(2*n)+[pl.BlockSpec((NH*E,D),lambda s:(0,0))]+[any_]*len(extra),
        out_specs=pl.BlockSpec((NH*E,2*BLK),lambda s:(0,s+first)),out_shape=jax.ShapeDtypeStruct((NH*E,T),bf16),
        scratch_shapes=[pltpu.VMEM((n,2*BLK,D),bf16),pltpu.SemaphoreType.DMA((2*n,))],input_output_aliases={2*n+1:0} if extra else {},
        compiler_params=pltpu.CompilerParams(dimension_semantics=("arbitrary",),vmem_limit_bytes=24<<20),
        cost_estimate=pl.CostEstimate(flops=n*512*D*NH*E*2,bytes_accessed=10<<20,transcendentals=0))(*pieces,wo,*extra)

def solution(mesh):
    def layer(x_in, x_mid, d_out, q_saved, k_saved, v_saved, z_saved, g1, b1, g2, b2, w_qkv, w_proj, w_fc1, w_fc2):
        me=lax.axis_index('tp').astype(jnp.int32)
        me1=jnp.reshape(me,(1,))
        p8=jnp.arange(8,dtype=jnp.int32)
        blk=lax.bitwise_xor(me,2*turn(p8//2,me%2)+p8%2)
        x_in, x_mid, d_out, z = x_in[0], x_mid[0], d_out[0], z_saved[0]
        heads=lambda a: a[0].transpose(1,2,0)
        q,k,v=heads(q_saved),heads(k_saved),heads(v_saved)
        wqkv=w_qkv.transpose(0,2,3,1).reshape(3*NH*E,D)
        wo=w_proj.reshape(NH*E,D)
        dya,dyb,dyp=hop_a(d_out),hop_b(d_out),partner(d_out)
        u,slope=gelu(blk,z)
        dz,db_0,(o0,o1)=mlp(0,[d_out,dyp],slope,w_fc2,w_fc1,None)
        dya=after(dya,db_0)
        dyd=hop_b(dya)
        h2_local=layer_norm_fwd(after(x_mid,dya),g2,b2)
        h2a,h2b,h2p=hop_a(h2_local),hop_b(h2_local),partner(h2_local)
        dypa,dypb=partner(dya),partner(dyb)
        dz,db_1,(pa0,pa1,pb0,pb1)=mlp(1,[dya,dypb,dyb,dypa],slope,w_fc2,w_fc1,dz)
        ra,rb,ro=partner(pb1),partner(pa1),partner(o1)
        a_in=hop_a(add2(pa0,ra))
        dypd=partner(dyd)
        dz,db_2,(pd0,pd1)=mlp(3,[dyd,dypd],slope,w_fc2,w_fc1,dz)
        d_sum=add2(pd0,partner(pd1))
        d_in=hop_a(d_sum)
        ctx,lse01=attn_fwd(0,2,me1,after(q,d_sum),k,v,None)
        b_sum=(pb0.astype(f32)+after(rb,lse01).astype(f32)+d_in.astype(f32)).astype(bf16)
        b_in=hop_b(b_sum)
        h2a=after(h2a,b_sum)
        h2d=hop_b(h2a); h2pa,h2pb=partner(h2a),partner(h2b)
        ctx,lse2=attn_fwd(2,1,me1,after(q,b_sum),k,v,ctx)
        mid,vec2=ln_bwd((after(o0,lse2),ro,a_in,b_in),x_mid,d_out,g2)
        grad_bfc1=jnp.sum(db_0+db_1+db_2,axis=0)
        dxa,dxb,dxp=hop_a(mid),hop_b(mid),partner(mid)
        dys=[d_out,dyp,dya,dypb,dyb,dypa,dyd,dypd]
        grad_wfc2=gathered_mm(lambda x,o: tn(o[...],x,0,0),dys,after(u,mid),9,
            pl.BlockSpec((F,256),lambda s:(0,s)),jax.ShapeDtypeStruct((F,D),f32),2*T*D*F)
        h1_local=layer_norm_fwd(after(x_in,mid),g1,b1)
        dxa=after(dxa,grad_wfc2,h1_local)
        dxd=hop_b(dxa)
        dxpa,dxpb=partner(dxa),partner(dxb)
        h2pd=partner(after(h2d,grad_wfc2))
        h2=[h2_local,h2p,h2a,h2pb,h2b,h2pa,h2d,h2pd]
        grad_wfc1=gathered_mm(lambda x,o: tn(x,o[...],0,0),h2,after(dz,dxa),3,
            pl.BlockSpec((768,F),lambda s:(s,0)),jax.ShapeDtypeStruct((D,F),f32),2*T*D*F)
        dctx=ctx_grad(0,[mid,dxp,dxa,dxpb,dxb,dxpa],after(wo,grad_wfc1),None)
        dxd=after(dxd,dctx)
        dxpd=partner(dxd)
        h1_local=after(h1_local,dxd)
        h1a,h1b,h1p=hop_a(h1_local),hop_b(h1_local),partner(h1_local)
        dx1=[mid,dxp,dxa,dxpb,dxb,dxpa,dxd,dxpd]
        dctx=ctx_grad(3,[dxd,dxpd],wo,dctx).reshape(NH,E,T)
        dqkv=attn_bwd(0,2,me1,q,k,v,dctx,lse01,None)
        h1a=after(h1a,dqkv)
        h1d=hop_b(h1a); h1pa,h1pb=partner(h1a),partner(h1b)
        dqkv=attn_bwd(2,1,me1,q,k,v,dctx,lse2,dqkv)
        dqkv=dqkv.reshape(3*NH*E,T)
        pd0,pd1,pa0,pa1=attn_in_grad((3,1),dqkv,wqkv)
        d_sum=add2(pd0,partner(pd1))
        d_in=hop_a(d_sum)
        rb=partner(pa1)
        pb0,pb1,o0,o1=attn_in_grad((2,0),after(dqkv,d_sum),wqkv)
        ra,ro=partner(pb1),partner(o1)
        a_sum=add2(pa0,ra)
        a_in=hop_a(a_sum)
        b_sum=(pb0.astype(f32)+after(rb,a_sum).astype(f32)+d_in.astype(f32)).astype(bf16)
        b_in=hop_b(b_sum)
        h1pd=partner(after(h1d,dqkv))
        h1=[h1_local,h1p,h1a,h1pb,h1b,h1pa,h1d,h1pd]
        grad_wqkv=gathered_mm(lambda x,o: jnp.dot(o[...],x,preferred_element_type=f32),h1,after(dqkv,b_sum),3,
            pl.BlockSpec((3*NH*E,768),lambda s:(0,s)),jax.ShapeDtypeStruct((3*NH*E,D),f32),6*T*D*NH*E)
        dx,vec1=ln_bwd((after(o0,grad_wqkv),ro,a_in,b_in),x_in,mid,g1)
        grad_vecs=jnp.concatenate([vec1[:2],vec2],axis=0)
        def all_sum(vecs,k): return vecs+send(vecs,[(i,i^k) for i in range(8)])
        vecs=all_sum(grad_vecs,1)
        grad_wproj=gathered_mm(lambda x,o: jnp.dot(o[...],x,preferred_element_type=f32),dx1,after(ctx,dx).reshape(NH*E,T),3,
            pl.BlockSpec((NH*E,768),lambda s:(0,s)),jax.ShapeDtypeStruct((NH*E,D),f32),2*T*D*NH*E)
        vecs=all_sum(after(vecs,grad_wproj),2)
        grad_bqkv=jnp.sum(after(dqkv,grad_wproj),axis=1,dtype=f32).reshape(3,NH,E)
        grad_vecs=all_sum(vecs,4)
        grad_wproj=grad_wproj.reshape(NH,E,D)
        grad_wqkv=grad_wqkv.reshape(3,NH,E,D).transpose(0,3,1,2)
        return dx[None], grad_wqkv, grad_bqkv, grad_wproj, grad_wfc1, grad_bfc1, grad_wfc2, grad_vecs

    tok_spec = P('dp', 'tp', None)
    head_spec = P('dp', None, 'tp', None)
    in_specs = (tok_spec, tok_spec, tok_spec, head_spec, head_spec, head_spec, P('dp', None, 'tp'),
                P(None), P(None), P(None), P(None),
                P(None, None, 'tp', None), P('tp', None, None), P(None, 'tp'), P('tp', None))
    out_specs = (tok_spec, P('dp', None, 'tp', None), P('dp', 'tp', None), P(('dp', 'tp'), None, None),
                 P('dp', 'tp'), P(('dp', 'tp')), P(('dp', 'tp'), None), P('dp', None))
    return jax.shard_map(layer, mesh=mesh, in_specs=in_specs, out_specs=out_specs, check_vma=False)
```

```python
import jax, jax.numpy as jnp
from jax import lax
from jax.experimental import pallas as pl
from jax.experimental.pallas import tpu as pltpu
from jax.sharding import PartitionSpec as P
T=2048; E=96; NH=3; BQ=512; NQ=T//BQ; BLK=256
C=E**-0.5; C2=C*1.4426950408889634
f32=jnp.float32; bf16=jnp.bfloat16

def turn(h, core):
    return jnp.where(core==0, h, (h%2)*2+h//2)

def rel_pos(block, me):
    j=lax.bitwise_xor(block, me)
    return 2*turn(j//2, me%2)+j%2

def tn(a,b,ca,cb): return lax.dot_general(a,b,(((ca,),(cb,)),((),())),preferred_element_type=f32)

def fold8(a): return jnp.sum(a.reshape(a.shape[0]//8,8,a.shape[1]),axis=0)
def foldmax8(a): return jnp.max(a.reshape(a.shape[0]//8,8,a.shape[1]),axis=0)

def causal(s, fill):
    r=lax.broadcasted_iota(jnp.int32,s.shape,0); c=lax.broadcasted_iota(jnp.int32,s.shape,1)
    return jnp.where(r<=c,s,fill)

def fwd_kernel(me_ref,q_ref,k_ref,v_ref,_,ctx_ref,lse_ref,kt,sc,acc,m8):
    i=pl.program_id(1)
    @pl.when(i==0)
    def _(): kt[...]=k_ref[0].T
    q=q_ref[0]
    def rows(j): return pl.ds(pl.multiple_of(j*BQ,BQ),BQ)
    halves=[(pl.ds(pl.multiple_of(i*BQ+c,BLK),BLK),c) for c in (0,BLK)]
    def p1(j,m):
        s=jnp.dot(kt[rows(j),:],q,preferred_element_type=f32)
        sc[rows(j),:]=s
        return jnp.maximum(m,foldmax8(s))
    m8[...]=lax.fori_loop(0,i,p1,jnp.full((8,BQ),-1e30,f32))
    for r,c in halves:
        s=causal(jnp.dot(kt[r,:],q[:,c:],preferred_element_type=f32),-1e30)
        sc[r,c:]=s
        m8[:,c:]=jnp.maximum(m8[:,c:],foldmax8(s))
    m=jnp.max(m8[...],axis=0,keepdims=True)*C2
    def p2(j,l):
        e=jnp.exp2(sc[rows(j),:]*C2-m)
        sc[rows(j),:]=e
        return l+fold8(e)
    m8[...]=lax.fori_loop(0,i,p2,jnp.zeros((8,BQ),f32))
    for r,c in halves:
        e=jnp.exp2(sc[r,c:]*C2-m[:,c:])
        sc[r,c:]=e
        m8[:,c:]+=fold8(e)
    l=jnp.sum(m8[...],axis=0,keepdims=True)
    inv=1.0/l
    lse_ref[0]=m+jnp.log2(l)
    acc[...]=jnp.zeros_like(acc)
    def p3(j,_):
        p=(sc[rows(j),:]*inv).astype(bf16)
        acc[...]+=jnp.dot(v_ref[0,:,rows(j)],p,preferred_element_type=f32)
        return 0
    lax.fori_loop(0,i,p3,0)
    for r,c in halves:
        acc[:,c:]+=jnp.dot(v_ref[0,:,r],(sc[r,c:]*inv[:,c:]).astype(bf16),preferred_element_type=f32)
    for a in range(BQ//BLK):
        pos=rel_pos(i*(BQ//BLK)+a,me_ref[0])
        ctx_ref[0,:,pl.ds(pl.multiple_of(pos*BLK,BLK),BLK)]=acc[:,a*BLK:(a+1)*BLK].astype(bf16)

def bwd_kernel(me_ref,q_ref,k_ref,v_ref,g_ref,lse_ref,_,out_ref,kt,vt,psc,dsc,g_sc,dq,dk,dv,d8):
    i=pl.program_id(1)
    @pl.when(i==0)
    def _():
        kt[...]=k_ref[0].T
        vt[...]=v_ref[0].T
        dk[...]=jnp.zeros_like(dk); dv[...]=jnp.zeros_like(dv)
    def rows(j): return pl.ds(pl.multiple_of(j*BQ,BQ),BQ)
    for a in range(BQ//BLK):
        pos=rel_pos(i*(BQ//BLK)+a,me_ref[0])
        g_sc[:,a*BLK:(a+1)*BLK]=g_ref[0,:,pl.ds(pl.multiple_of(pos*BLK,BLK),BLK)]
    q=q_ref[0]; g=g_sc[...]; lse=lse_ref[0]
    halves=[(pl.ds(pl.multiple_of(i*BQ+c,BLK),BLK),c) for c in (0,BLK)]
    def tile(r,c,diag):
        s=jnp.dot(kt[r,:],q[:,c:],preferred_element_type=f32)
        p=jnp.exp2(s*C2-lse[:,c:])
        if diag: p=causal(p,0.0)
        dp=jnp.dot(vt[r,:],g[:,c:],preferred_element_type=f32)
        psc[r,c:]=p; dsc[r,c:]=dp
        return fold8(p*dp)
    d8[...]=lax.fori_loop(0,i,lambda j,d: d+tile(rows(j),0,False),jnp.zeros((8,BQ),f32))
    for r,c in halves: d8[:,c:]+=tile(r,c,True)
    delta=jnp.sum(d8[...],axis=0,keepdims=True)
    dq[...]=jnp.zeros_like(dq)
    def grads(r,c):
        p=psc[r,c:]
        ds=(p*(dsc[r,c:]-delta[:,c:])*C).astype(bf16)
        dq[:,c:]+=jnp.dot(k_ref[0,:,r],ds,preferred_element_type=f32)
        dk[:,r]+=tn(q[:,c:],ds,1,1)
        dv[:,r]+=tn(g[:,c:],p.astype(bf16),1,1)
    def p2(j,_):
        grads(rows(j),0)
        return 0
    lax.fori_loop(0,i,p2,0)
    for r,c in halves: grads(r,c)
    for a in range(BQ//BLK):
        pos=rel_pos(i*(BQ//BLK)+a,me_ref[0])
        out_ref[0,0,:,pl.ds(pl.multiple_of(pos*BLK,BLK),BLK)]=dq[:,a*BLK:(a+1)*BLK].astype(bf16)
    @pl.when(i==NQ-1)
    def _():
        for b in range(T//BLK):
            at=pl.ds(pl.multiple_of(rel_pos(b,me_ref[0])*BLK,BLK),BLK)
            out_ref[1,0,:,at]=dk[:,b*BLK:(b+1)*BLK].astype(bf16)
            out_ref[2,0,:,at]=dv[:,b*BLK:(b+1)*BLK].astype(bf16)

NEL=(NQ*(NQ+1)//2)*BQ*BQ
def attn_call(kernel, n, ins, in_specs, out_specs, out_shape, scratch, flops, prev):
    al={}
    if prev is None: prev=ins[0]
    else: al={len(ins):0}
    return pl.pallas_call(kernel,
        grid_spec=pltpu.PrefetchScalarGridSpec(num_scalar_prefetch=1,grid=(n,NQ),
            in_specs=in_specs+[pl.BlockSpec(memory_space=pl.ANY if al else pltpu.SMEM)],out_specs=out_specs,scratch_shapes=scratch),
        out_shape=out_shape,input_output_aliases=al,
        compiler_params=pltpu.CompilerParams(dimension_semantics=("arbitrary","arbitrary"),vmem_limit_bytes=40<<20),
        cost_estimate=pl.CostEstimate(flops=n*flops,bytes_accessed=n*(3<<20),transcendentals=n*NEL))(*ins,prev)
def head_specs(h0):
    full=pl.BlockSpec((1,E,T),lambda h,i,me:(h+h0,0,0))
    return full,pl.BlockSpec((1,E,BQ),lambda h,i,me:(h+h0,0,i)),pl.BlockSpec((1,1,BQ),lambda h,i,me:(h,0,i))
def attn_fwd(h0,n,me,q,k,v,prev):
    full,qblk,lblk=head_specs(h0)
    return attn_call(fwd_kernel,n,(me,q,k,v),[qblk,full,full],[full,lblk],
        [jax.ShapeDtypeStruct((NH,E,T),bf16),jax.ShapeDtypeStruct((n,1,T),f32)],
        [pltpu.VMEM((T,E),bf16),pltpu.VMEM((T,BQ),f32),pltpu.VMEM((E,BQ),f32),pltpu.VMEM((8,BQ),f32)],NEL*1024,prev)
def attn_bwd(h0,n,me,q,k,v,g,lse,prev):
    full,qblk,lblk=head_specs(h0)
    return attn_call(bwd_kernel,n,(me,q,k,v,g,lse),[qblk,full,full,full,lblk],
        pl.BlockSpec((3,1,E,T),lambda h,i,me:(0,h+h0,0,0)),jax.ShapeDtypeStruct((3,NH,E,T),bf16),
        [pltpu.VMEM((T,E),bf16),pltpu.VMEM((T,E),bf16),pltpu.VMEM((T,BQ),f32),pltpu.VMEM((T,BQ),f32),
         pltpu.VMEM((E,BQ),bf16),pltpu.VMEM((E,BQ),f32),pltpu.VMEM((E,T),f32),pltpu.VMEM((E,T),f32),pltpu.VMEM((8,BQ),f32)],NEL*2048,prev)

LN_EPS=1e-5
GELU_COEF=0.044715
GELU_SCALE=0.7978845608028654
D=2304
F=1152
ANY=pl.ANY

def send(a, pairs):
    return lax.ppermute(a, 'tp', pairs)
def partner(a): return send(a, [(i, i ^ 1) for i in range(8)])
def hop_a(a):
    return send(a, [(i, i ^ (2 if i % 2 == 0 else 4)) for i in range(8)])
def hop_b(a): return send(a, [(i, i ^ (4 if i % 2 == 0 else 2)) for i in range(8)])
def after(x, *deps): return lax.optimization_barrier((x,)+deps)[0]

def add2(a, b): return (a.astype(f32)+b.astype(f32)).astype(bf16)

def ln_fwd_kernel(rows, gain, bias, out):
    r=rows[...].astype(f32)
    cen=r-jnp.mean(r,axis=-1,keepdims=True)
    rstd=lax.rsqrt(jnp.mean(cen*cen,axis=-1,keepdims=True)+LN_EPS)
    out[...]=(cen*rstd*gain[...]+bias[...]).astype(bf16)

def layer_norm_fwd(rows, gain, bias):
    R=64
    blk=pl.BlockSpec((R,D),lambda i:(i,0)); vec=pl.BlockSpec((1,D),lambda i:(0,0))
    return pl.pallas_call(ln_fwd_kernel,grid=(256//R,),in_specs=[blk,vec,vec],out_specs=blk,out_shape=jax.ShapeDtypeStruct((256,D),bf16),
        compiler_params=pltpu.CompilerParams(dimension_semantics=("arbitrary",),vmem_limit_bytes=16<<20),
        cost_estimate=pl.CostEstimate(flops=256*D*1000,bytes_accessed=3<<20,transcendentals=0))(rows,gain.reshape(1,D),bias.reshape(1,D))

def ln_bwd_kernel(own, ro, a_in, *refs):
    rows, skip, gain, more, out, total, vec=refs[-7:]
    i=pl.program_id(0)
    b_in=refs[0][...].astype(f32) if len(refs)==8 else jnp.where(i<2,refs[0][...].astype(f32),refs[1][...].astype(f32))
    dh=(own[...].astype(f32)+ro[...].astype(f32))+(a_in[...].astype(f32)+b_in)
    r=rows[...].astype(f32)
    cen=r-jnp.mean(r,axis=-1,keepdims=True)
    rstd=lax.rsqrt(jnp.mean(cen*cen,axis=-1,keepdims=True)+LN_EPS)
    hat=cen*rstd
    gh=dh*gain[...]
    cg=gh-jnp.mean(gh,axis=-1,keepdims=True)
    sk=skip[...].astype(f32)
    o=(sk+rstd*(cg-hat*jnp.mean(gh*hat,axis=-1,keepdims=True))).astype(bf16)
    out[...]=o
    @pl.when(i==0)
    def _(): vec[...]=jnp.zeros_like(vec)
    vec[0]+=fold8(dh*hat); vec[1]+=fold8(dh)
    if total.shape[0]==4: vec[2]+=fold8(o.astype(f32)); vec[3]+=fold8(sk)
    @pl.when(i==3)
    def _():
        for k in range(2 if total.shape[0]==6 else 4): total[k:k+1,:]=jnp.sum(vec[k],axis=0,keepdims=True)
        if total.shape[0]==6: total[2:6,:]=more[...]

def ln_bwd(parts, rows, skip, gain, more):
    R=64
    blk=pl.BlockSpec((R,D),lambda i:(i,0))
    n=6 if more.shape[0]==4 else 4
    b_specs=[blk] if len(parts)==4 else [pl.BlockSpec((R,D),lambda i:(jnp.minimum(i,1),0)),pl.BlockSpec((R,D),lambda i:(jnp.maximum(i-2,0),0))]
    out,vec=pl.pallas_call(ln_bwd_kernel,grid=(256//R,),
        in_specs=[blk]*3+b_specs+[blk]*2+[pl.BlockSpec((1,D),lambda i:(0,0)),pl.BlockSpec(more.shape,lambda i:(0,0))],
        out_specs=[blk,pl.BlockSpec((n,D),lambda i:(0,0))],scratch_shapes=[pltpu.VMEM((4,8,D),f32)],
        out_shape=[jax.ShapeDtypeStruct((256,D),bf16),jax.ShapeDtypeStruct((n,D),f32)],
        compiler_params=pltpu.CompilerParams(dimension_semantics=("arbitrary",),vmem_limit_bytes=16<<20),
        cost_estimate=pl.CostEstimate(flops=256*D*1000,bytes_accessed=6<<20,transcendentals=0))(*parts,rows,skip,gain.reshape(1,D),more)
    return out,vec

def join(a, b):
    def kernel(a, b, out):
        out[0]=a[0]; out[1]=b[0]
    return pl.pallas_call(kernel,name="lse_join",out_shape=jax.ShapeDtypeStruct((2,1,T),f32),compiler_params=pltpu.CompilerParams(vmem_limit_bytes=4<<20),
        cost_estimate=pl.CostEstimate(flops=T*100,bytes_accessed=8*T,transcendentals=0))(a,b)

def call(kernel, grid, in_specs, out_specs, out_shape, scratch, flops, args):
    return pl.pallas_call(kernel,grid=grid,in_specs=in_specs,out_specs=out_specs,out_shape=out_shape,
        scratch_shapes=scratch,compiler_params=pltpu.CompilerParams(dimension_semantics=("arbitrary",)*len(grid),vmem_limit_bytes=40<<20),
        cost_estimate=pl.CostEstimate(flops=flops,bytes_accessed=30<<20,transcendentals=0))(*args)

RB=256; SUB=BLK//RB
def mlp(first, blk, pieces, z, w2, w1, prev):
    n=len(pieces)//2
    def kernel(*refs):
        dy=refs[1:1+2*n]; z_ref,w2h,w1h=refs[1+2*n:4+2*n]
        refs=refs[2*n+(4 if prev is None else 6):]
        dz_ref,u_ref,db_ref=refs[:3]; dh=refs[3:3+2*n]
        x,w2s,w1s,st,xsem,wsem,osem=refs[3+2*n:]
        s=pl.program_id(0)
        class wcopy:
            def __init__(self, k):
                h,v=((w2h,w2s),(w1h,w1s))[k]
                r=v.shape[0]//4
                self.cs=[pltpu.make_async_copy(h.at[j*r:(j+1)*r],v.at[j*r:(j+1)*r],wsem.at[k,j]) for j in range(4)]
            def start(self):
                for c in self.cs: c.start()
            def wait(self):
                for c in self.cs: c.wait()
        def xcopy(p): return pltpu.make_async_copy(dy[p],x.at[p*BLK:(p+1)*BLK],xsem.at[p])
        def ocopy(p): return pltpu.make_async_copy(st.at[p*BLK:(p+1)*BLK],dh[p],osem.at[p])
        @pl.when(s==0)
        def _():
            xcopy(0).start()
            wcopy(0).start()
            for p in range(1,2*n): xcopy(p).start()
            wcopy(1).start()
            db_ref[...]=jnp.zeros_like(db_ref)
            wcopy(0).wait()
        for k in range(2*n):
            @pl.when(s==k*SUB)
            def _(): xcopy(k).wait()
        rows=pl.ds(pl.multiple_of(s*RB,RB),RB)
        zf=z_ref[...].astype(f32)
        t=zf*zf
        th=jnp.tanh(zf*(GELU_SCALE*GELU_COEF*t+GELU_SCALE))
        hz=0.5*zf
        u_ref[...]=(hz*th+hz).astype(bf16)
        slope=(0.5*th+0.5)+hz*(1.0-th*th)*(3.0*GELU_SCALE*GELU_COEF*t+GELU_SCALE)
        dz=(tn(x[rows,:],w2s[...],1,1)*slope).astype(bf16)
        dz_ref[...]=dz
        db_ref[...]+=fold8(dz.astype(f32))
        @pl.when(s==0)
        def _(): wcopy(1).wait()
        if first>0: st[rows,:]=tn(dz_ref[...],w1s[...],1,1).astype(bf16)
        else:
            def part(c,_):
                at=pl.ds(pl.multiple_of(c*768,768),768)
                st[rows,at]=tn(dz_ref[...],w1s[at,:],1,1).astype(bf16)
                return 0
            lax.fori_loop(0,3,part,0)
        for k in range(2*n):
            @pl.when(s==k*SUB+SUB-1)
            def _(): ocopy(k).start()
        @pl.when(s==2*n*SUB-1)
        def _():
            for p in range(2*n): ocopy(p).wait()
    any_=pl.BlockSpec(memory_space=ANY)
    step=pl.BlockSpec((RB,F),lambda s,blk:(s+2*first*SUB,0))
    extra=() if prev is None else prev
    outs=pl.pallas_call(kernel,
        grid_spec=pltpu.PrefetchScalarGridSpec(num_scalar_prefetch=1,grid=(2*n*SUB,),
            in_specs=[any_]*(2*n)+[pl.BlockSpec((RB,F),lambda s,blk:(blk[s//SUB+2*first]*SUB+s%SUB,0))]+[any_]*(2+len(extra)),
            out_specs=[step,step,pl.BlockSpec((8,F),lambda s,blk:(0,0))]+[any_]*(2*n),
            scratch_shapes=[pltpu.VMEM((2*n*BLK,D),bf16),pltpu.VMEM((F,D),bf16),pltpu.VMEM((D,F),bf16),pltpu.VMEM((2*n*BLK,D),bf16),
             pltpu.SemaphoreType.DMA((2*n,)),pltpu.SemaphoreType.DMA((2,4)),pltpu.SemaphoreType.DMA((2*n,))]),
        out_shape=[jax.ShapeDtypeStruct((T,F),bf16)]*2+[jax.ShapeDtypeStruct((8,F),f32)]+[jax.ShapeDtypeStruct((BLK,D),bf16)]*(2*n),
        input_output_aliases={2*n+4+k:k for k in range(len(extra))},
        compiler_params=pltpu.CompilerParams(dimension_semantics=("arbitrary",),vmem_limit_bytes=48<<20),
        cost_estimate=pl.CostEstimate(flops=n*T*D*F,bytes_accessed=20<<20,transcendentals=0))(blk,*pieces,z,w2,w1,*extra)
    return (outs[0],outs[1]),outs[2],list(outs[3:])

def attn_in_grad(chips, dqkv, wqkv):
    c0,c1=chips
    def kernel(g,w,*refs):
        dh=refs[:4]; st,sem=refs[4:]
        s=pl.program_id(0)
        def ocopy(p): return pltpu.make_async_copy(st.at[p*BLK:(p+1)*BLK],dh[p],sem.at[p])
        rows=pl.ds(pl.multiple_of(s*BLK,BLK),BLK)
        st[rows,:]=tn(g[...],w[...],0,0).astype(bf16)
        for k in range(4):
            @pl.when(s==k)
            def _(): ocopy(k).start()
        @pl.when(s==3)
        def _():
            for p in range(4): ocopy(p).wait()
    K=3*NH*E
    return call(kernel,(4,),[pl.BlockSpec((K,BLK),lambda s:(0,2*(c0+(c1-c0)*(s//2))+s%2)),pl.BlockSpec((K,D),lambda s:(0,0))],
        [pl.BlockSpec(memory_space=ANY)]*4,[jax.ShapeDtypeStruct((BLK,D),bf16)]*4,
        [pltpu.VMEM((4*BLK,D),bf16),pltpu.SemaphoreType.DMA((4,))],T*D*K,(dqkv,wqkv))

def gathered_mm(body, pieces, other, n, out_spec, out_shape, flops, cols=(0,D), into=None):
    W=(cols[1]-cols[0])//n
    def kernel(*refs):
        ps=refs[:8]; o_ref=refs[8]; out,full,sem=refs[-3:]
        s=pl.program_id(0)
        def copy(t,p): return pltpu.make_async_copy(ps[p].at[:,cols[0]+t*W:cols[0]+(t+1)*W],full.at[t,p*BLK:(p+1)*BLK],sem.at[t,p])
        @pl.when(s==0)
        def _():
            for t in range(n):
                for p in range(8): copy(t,p).start()
        for t in range(n):
            @pl.when(s==t)
            def _():
                for p in range(8): copy(t,p).wait()
        out[...]=body(full[s],o_ref)
    any_=pl.BlockSpec(memory_space=ANY)
    extra=() if into is None else (into,)
    return pl.pallas_call(kernel,grid=(n,),in_specs=[any_]*8+[pl.BlockSpec(other.shape,lambda s:(0,0))]+[any_]*len(extra),out_specs=out_spec,out_shape=out_shape,
        scratch_shapes=[pltpu.VMEM((n,T,W),bf16),pltpu.SemaphoreType.DMA((n,8))],input_output_aliases={9:0} if extra else {},
        compiler_params=pltpu.CompilerParams(dimension_semantics=("arbitrary",),vmem_limit_bytes=60<<20),
        cost_estimate=pl.CostEstimate(flops=flops,bytes_accessed=30<<20,transcendentals=0))(*pieces,other,*extra)

def ctx_grad(first, pieces, wo, into):
    n=len(pieces)//2
    def kernel(*refs):
        ps=refs[:2*n]; w=refs[2*n]; out,full,sem=refs[-3:]
        s=pl.program_id(0)
        def copy(p): return pltpu.make_async_copy(ps[p],full.at[p//2,(p%2)*BLK:(p%2+1)*BLK],sem.at[p])
        @pl.when(s==0)
        def _():
            for p in range(2*n): copy(p).start()
        for k in range(n):
            @pl.when(s==k)
            def _():
                copy(2*k).wait(); copy(2*k+1).wait()
        out[...]=tn(w[...],full[s],1,1).astype(bf16)
    any_=pl.BlockSpec(memory_space=ANY)
    extra=() if into is None else (into,)
    return pl.pallas_call(kernel,grid=(n,),in_specs=[any_]*(2*n)+[pl.BlockSpec((NH*E,D),lambda s:(0,0))]+[any_]*len(extra),
        out_specs=pl.BlockSpec((NH*E,2*BLK),lambda s:(0,s+first)),out_shape=jax.ShapeDtypeStruct((NH*E,T),bf16),
        scratch_shapes=[pltpu.VMEM((n,2*BLK,D),bf16),pltpu.SemaphoreType.DMA((2*n,))],input_output_aliases={2*n+1:0} if extra else {},
        compiler_params=pltpu.CompilerParams(dimension_semantics=("arbitrary",),vmem_limit_bytes=24<<20),
        cost_estimate=pl.CostEstimate(flops=n*512*D*NH*E*2,bytes_accessed=10<<20,transcendentals=0))(*pieces,wo,*extra)

def solution(mesh):
    def layer(x_in, x_mid, d_out, q_saved, k_saved, v_saved, z_saved, g1, b1, g2, b2, w_qkv, w_proj, w_fc1, w_fc2):
        me=lax.axis_index('tp').astype(jnp.int32)
        me1=jnp.reshape(me,(1,))
        p8=jnp.arange(8,dtype=jnp.int32)
        blk=lax.bitwise_xor(me,2*turn(p8//2,me%2)+p8%2)
        x_in, x_mid, d_out, z = x_in[0], x_mid[0], d_out[0], z_saved[0]
        heads=lambda a: a[0].transpose(1,2,0)
        q,k,v=heads(q_saved),heads(k_saved),heads(v_saved)
        wqkv=w_qkv.transpose(0,2,3,1).reshape(3*NH*E,D)
        wo=w_proj.reshape(NH*E,D)
        dya,dyb,dyp=hop_a(d_out),hop_b(d_out),partner(d_out)
        dzu,db_0,(o0,o1)=mlp(0,blk,[d_out,dyp],z,w_fc2,w_fc1,None)
        h2_local=layer_norm_fwd(after(x_mid,db_0),g2,b2)
        ctx,lse0=attn_fwd(0,1,me1,after(q,db_0),k,v,None)
        dya=after(dya,lse0,h2_local)
        dyd=hop_b(dya)
        h2_local=after(h2_local,dya)
        h2a,h2b,h2p=hop_a(h2_local),hop_b(h2_local),partner(h2_local)
        dypa,dypb=partner(dya),partner(dyb)
        dzu,db_1,(pa0,pa1,pb0,pb1)=mlp(1,blk,[dya,dypb,dyb,dypa],z,w_fc2,w_fc1,dzu)
        ra,rb,ro=partner(pb1),partner(pa1),partner(o1)
        a_in=hop_a(add2(pa0,ra))
        dypd=partner(dyd)
        (dz,u),db_2,(pd0,pd1)=mlp(3,blk,[dyd,dypd],z,w_fc2,w_fc1,dzu)
        rd=partner(pd1)
        d_sum=[add2(pd0[:128],rd[:128]),add2(pd0[128:],rd[128:])]
        d_in=[hop_a(d_sum[0]),hop_a(d_sum[1])]
        def b_half(k,lse): return (pb0[128*k:128*k+128].astype(f32)+after(rb,lse)[128*k:128*k+128].astype(f32)+d_in[k].astype(f32)).astype(bf16)
        ctx,lse1=attn_fwd(1,1,me1,after(q,*d_sum),k,v,ctx)
        b_sum=b_half(0,lse1)
        b_in0=hop_b(b_sum)
        b_sum=b_half(1,b_sum)
        b_in1=hop_b(b_sum)
        ctx,lse2=attn_fwd(2,1,me1,after(q,b_sum),k,v,ctx)
        lse01=join(lse0,lse1)
        h2a=after(h2a,b_sum)
        h2d=hop_b(h2a); h2pa,h2pb=partner(h2a),partner(h2b)
        mid,vec2=ln_bwd((after(o0,lse2),ro,a_in,b_in0,b_in1),x_mid,d_out,g2,g2.reshape(1,D))
        grad_bfc1=jnp.sum(db_0+db_1+db_2,axis=0)
        dxa,dxb,dxp=hop_a(mid),hop_b(mid),partner(mid)
        dys=[d_out,dyp,dya,dypb,dyb,dypa,dyd,dypd]
        grad_wfc2=gathered_mm(lambda x,o: tn(o[...],x,0,0),dys,after(u,mid),9,
            pl.BlockSpec((F,256),lambda s:(0,s)),jax.ShapeDtypeStruct((F,D),f32),2*T*D*F)
        h2pd=partner(after(h2d,grad_wfc2))
        h2=[h2_local,h2p,h2a,h2pb,h2b,h2pa,h2d,h2pd]
        h1_local=layer_norm_fwd(after(x_in,grad_wfc2),g1,b1)
        def w1_part(c0,n,left,into):
            return gathered_mm(lambda x,o: tn(x,o[...],0,0),h2,left,n,
                pl.BlockSpec((256,F),lambda s:(s+c0,0)),jax.ShapeDtypeStruct((D,F),f32),2*T*256*n*F,cols=(256*c0,256*(c0+n)),into=into)
        grad_wfc1=w1_part(0,3,after(dz,h1_local),None)
        dxa=after(dxa,grad_wfc1)
        dxd=hop_b(dxa)
        dxpa,dxpb=partner(dxa),partner(dxb)
        grad_wfc1=w1_part(3,6,after(dz,dxa),grad_wfc1)
        dctx=ctx_grad(0,[mid,dxp,dxa,dxpb,dxb,dxpa],after(wo,grad_wfc1),None)
        dxd=after(dxd,dctx)
        dxpd=partner(dxd)
        h1_local=after(h1_local,dxd)
        h1a,h1b,h1p=hop_a(h1_local),hop_b(h1_local),partner(h1_local)
        dx1=[mid,dxp,dxa,dxpb,dxb,dxpa,dxd,dxpd]
        dctx=ctx_grad(3,[dxd,dxpd],wo,dctx).reshape(NH,E,T)
        dqkv=attn_bwd(0,2,me1,q,k,v,dctx,lse01,None)
        h1a=after(h1a,dqkv)
        h1d=hop_b(h1a); h1pa,h1pb=partner(h1a),partner(h1b)
        dqkv=attn_bwd(2,1,me1,q,k,v,dctx,lse2,dqkv)
        dqkv=dqkv.reshape(3*NH*E,T)
        pd0,pd1,pa0,pa1=attn_in_grad((3,1),dqkv,wqkv)
        d_sum=add2(pd0,partner(pd1))
        d_in=hop_a(d_sum)
        rb=partner(pa1)
        pb0,pb1,o0,o1=attn_in_grad((2,0),after(dqkv,d_sum),wqkv)
        ra,ro=partner(pb1),partner(o1)
        a_sum=add2(pa0,ra)
        a_in=hop_a(a_sum)
        b_sum=(pb0.astype(f32)+after(rb,a_sum).astype(f32)+d_in.astype(f32)).astype(bf16)
        b_in=hop_b(b_sum)
        h1pd=partner(after(h1d,dqkv))
        h1=[h1_local,h1p,h1a,h1pb,h1b,h1pa,h1d,h1pd]
        grad_wqkv=gathered_mm(lambda x,o: jnp.dot(o[...],x,preferred_element_type=f32),h1,after(dqkv,b_sum),3,
            pl.BlockSpec((3*NH*E,768),lambda s:(0,s)),jax.ShapeDtypeStruct((3*NH*E,D),f32),6*T*D*NH*E)
        def wo_part(c0,n,left,into):
            return gathered_mm(lambda x,o: jnp.dot(o[...],x,preferred_element_type=f32),dx1,left,n,
                pl.BlockSpec((NH*E,256),lambda s:(0,s+c0)),jax.ShapeDtypeStruct((NH*E,D),f32),n*T*256*NH*E*2,cols=(256*c0,256*(c0+n)),into=into)
        ctx=ctx.reshape(NH*E,T)
        grad_wproj=wo_part(0,3,after(ctx,grad_wqkv),None)
        dx,grad_vecs=ln_bwd((after(o0,grad_wproj),ro,a_in,b_in),x_in,mid,g1,vec2)
        v2,v4,v6=(send(grad_vecs,[(i,i^k) for i in range(8)]) for k in (2,4,6))
        grad_wproj=wo_part(3,6,after(ctx,dx),grad_wproj)
        vecs=(grad_vecs+after(v2,grad_wproj))+(v4+v6)
        v1=send(vecs,[(i,i^1) for i in range(8)])
        grad_bqkv=jnp.sum(after(dqkv,vecs),axis=1,dtype=f32).reshape(3,NH,E)
        grad_vecs=vecs+v1
        grad_wproj=grad_wproj.reshape(NH,E,D)
        grad_wqkv=grad_wqkv.reshape(3,NH,E,D).transpose(0,3,1,2)
        return dx[None], grad_wqkv, grad_bqkv, grad_wproj, grad_wfc1, grad_bfc1, grad_wfc2, grad_vecs

    tok_spec = P('dp', 'tp', None)
    head_spec = P('dp', None, 'tp', None)
    in_specs = (tok_spec, tok_spec, tok_spec, head_spec, head_spec, head_spec, P('dp', None, 'tp'),
                P(None), P(None), P(None), P(None),
                P(None, None, 'tp', None), P('tp', None, None), P(None, 'tp'), P('tp', None))
    out_specs = (tok_spec, P('dp', None, 'tp', None), P('dp', 'tp', None), P(('dp', 'tp'), None, None),
                 P('dp', 'tp'), P(('dp', 'tp')), P(('dp', 'tp'), None), P('dp', None))
    return jax.shard_map(layer, mesh=mesh, in_specs=in_specs, out_specs=out_specs, check_vma=False)
```

```python
import jax, jax.numpy as jnp
from jax import lax
from jax.experimental import pallas as pl
from jax.experimental.pallas import tpu as pltpu
from jax.sharding import PartitionSpec as P
T=2048; E=96; NH=3; BQ=512; NQ=T//BQ; BLK=256
C=E**-0.5; C2=C*1.4426950408889634
f32=jnp.float32; bf16=jnp.bfloat16

def turn(h, core):
    return jnp.where(core==0, h, (h%2)*2+h//2)

def rel_pos(block, me):
    j=lax.bitwise_xor(block, me)
    return 2*turn(j//2, me%2)+j%2

def tn(a,b,ca,cb): return lax.dot_general(a,b,(((ca,),(cb,)),((),())),preferred_element_type=f32)

def fold8(a): return jnp.sum(a.reshape(a.shape[0]//8,8,a.shape[1]),axis=0)
def foldmax8(a): return jnp.max(a.reshape(a.shape[0]//8,8,a.shape[1]),axis=0)

def causal(s, fill):
    r=lax.broadcasted_iota(jnp.int32,s.shape,0); c=lax.broadcasted_iota(jnp.int32,s.shape,1)
    return jnp.where(r<=c,s,fill)

def fwd_kernel(me_ref,q_ref,k_ref,v_ref,_,ctx_ref,lse_ref,kt,sc,acc,m8):
    i=pl.program_id(1)
    @pl.when(i==0)
    def _(): kt[...]=k_ref[0].T
    q=q_ref[0]
    def rows(j): return pl.ds(pl.multiple_of(j*BQ,BQ),BQ)
    halves=[(pl.ds(pl.multiple_of(i*BQ+c,BLK),BLK),c) for c in (0,BLK)]
    def p1(j,m):
        s=jnp.dot(kt[rows(j),:],q,preferred_element_type=f32)
        sc[rows(j),:]=s
        return jnp.maximum(m,foldmax8(s))
    m8[...]=lax.fori_loop(0,i,p1,jnp.full((8,BQ),-1e30,f32))
    for r,c in halves:
        s=causal(jnp.dot(kt[r,:],q[:,c:],preferred_element_type=f32),-1e30)
        sc[r,c:]=s
        m8[:,c:]=jnp.maximum(m8[:,c:],foldmax8(s))
    m=jnp.max(m8[...],axis=0,keepdims=True)*C2
    def p2(j,l):
        e=jnp.exp2(sc[rows(j),:]*C2-m)
        sc[rows(j),:]=e
        return l+fold8(e)
    m8[...]=lax.fori_loop(0,i,p2,jnp.zeros((8,BQ),f32))
    for r,c in halves:
        e=jnp.exp2(sc[r,c:]*C2-m[:,c:])
        sc[r,c:]=e
        m8[:,c:]+=fold8(e)
    l=jnp.sum(m8[...],axis=0,keepdims=True)
    inv=1.0/l
    lse_ref[0]=m+jnp.log2(l)
    acc[...]=jnp.zeros_like(acc)
    def p3(j,_):
        p=(sc[rows(j),:]*inv).astype(bf16)
        acc[...]+=jnp.dot(v_ref[0,:,rows(j)],p,preferred_element_type=f32)
        return 0
    lax.fori_loop(0,i,p3,0)
    for r,c in halves:
        acc[:,c:]+=jnp.dot(v_ref[0,:,r],(sc[r,c:]*inv[:,c:]).astype(bf16),preferred_element_type=f32)
    for a in range(BQ//BLK):
        pos=rel_pos(i*(BQ//BLK)+a,me_ref[0])
        ctx_ref[0,:,pl.ds(pl.multiple_of(pos*BLK,BLK),BLK)]=acc[:,a*BLK:(a+1)*BLK].astype(bf16)

def bwd_kernel(me_ref,q_ref,k_ref,v_ref,g_ref,lse_ref,_,out_ref,kt,vt,psc,dsc,g_sc,dq,dk,dv,d8):
    i=pl.program_id(1)
    @pl.when(i==0)
    def _():
        kt[...]=k_ref[0].T
        vt[...]=v_ref[0].T
        dk[...]=jnp.zeros_like(dk); dv[...]=jnp.zeros_like(dv)
    def rows(j): return pl.ds(pl.multiple_of(j*BQ,BQ),BQ)
    for a in range(BQ//BLK):
        pos=rel_pos(i*(BQ//BLK)+a,me_ref[0])
        g_sc[:,a*BLK:(a+1)*BLK]=g_ref[0,:,pl.ds(pl.multiple_of(pos*BLK,BLK),BLK)]
    q=q_ref[0]; g=g_sc[...]; lse=lse_ref[0]
    halves=[(pl.ds(pl.multiple_of(i*BQ+c,BLK),BLK),c) for c in (0,BLK)]
    def tile(r,c,diag):
        s=jnp.dot(kt[r,:],q[:,c:],preferred_element_type=f32)
        p=jnp.exp2(s*C2-lse[:,c:])
        if diag: p=causal(p,0.0)
        dp=jnp.dot(vt[r,:],g[:,c:],preferred_element_type=f32)
        psc[r,c:]=p; dsc[r,c:]=dp
        return fold8(p*dp)
    d8[...]=lax.fori_loop(0,i,lambda j,d: d+tile(rows(j),0,False),jnp.zeros((8,BQ),f32))
    for r,c in halves: d8[:,c:]+=tile(r,c,True)
    delta=jnp.sum(d8[...],axis=0,keepdims=True)
    dq[...]=jnp.zeros_like(dq)
    def grads(r,c):
        p=psc[r,c:]
        ds=(p*(dsc[r,c:]-delta[:,c:])*C).astype(bf16)
        dq[:,c:]+=jnp.dot(k_ref[0,:,r],ds,preferred_element_type=f32)
        dk[:,r]+=tn(q[:,c:],ds,1,1)
        dv[:,r]+=tn(g[:,c:],p.astype(bf16),1,1)
    def p2(j,_):
        grads(rows(j),0)
        return 0
    lax.fori_loop(0,i,p2,0)
    for r,c in halves: grads(r,c)
    for a in range(BQ//BLK):
        pos=rel_pos(i*(BQ//BLK)+a,me_ref[0])
        out_ref[0,0,:,pl.ds(pl.multiple_of(pos*BLK,BLK),BLK)]=dq[:,a*BLK:(a+1)*BLK].astype(bf16)
    @pl.when(i==NQ-1)
    def _():
        for b in range(T//BLK):
            at=pl.ds(pl.multiple_of(rel_pos(b,me_ref[0])*BLK,BLK),BLK)
            out_ref[1,0,:,at]=dk[:,b*BLK:(b+1)*BLK].astype(bf16)
            out_ref[2,0,:,at]=dv[:,b*BLK:(b+1)*BLK].astype(bf16)

NEL=(NQ*(NQ+1)//2)*BQ*BQ
def attn_call(kernel, n, ins, in_specs, out_specs, out_shape, scratch, flops, prev):
    al={}
    if prev is None: prev=ins[0]
    else: al={len(ins):0}
    return pl.pallas_call(kernel,
        grid_spec=pltpu.PrefetchScalarGridSpec(num_scalar_prefetch=1,grid=(n,NQ),
            in_specs=in_specs+[pl.BlockSpec(memory_space=pl.ANY if al else pltpu.SMEM)],out_specs=out_specs,scratch_shapes=scratch),
        out_shape=out_shape,input_output_aliases=al,
        compiler_params=pltpu.CompilerParams(dimension_semantics=("arbitrary","arbitrary"),vmem_limit_bytes=40<<20),
        cost_estimate=pl.CostEstimate(flops=n*flops,bytes_accessed=n*(3<<20),transcendentals=n*NEL))(*ins,prev)
def head_specs(h0):
    full=pl.BlockSpec((1,E,T),lambda h,i,me:(h+h0,0,0))
    return full,pl.BlockSpec((1,E,BQ),lambda h,i,me:(h+h0,0,i)),pl.BlockSpec((1,1,BQ),lambda h,i,me:(h,0,i))
def attn_fwd(h0,n,me,q,k,v,prev):
    full,qblk,lblk=head_specs(h0)
    return attn_call(fwd_kernel,n,(me,q,k,v),[qblk,full,full],[full,lblk],
        [jax.ShapeDtypeStruct((NH,E,T),bf16),jax.ShapeDtypeStruct((n,1,T),f32)],
        [pltpu.VMEM((T,E),bf16),pltpu.VMEM((T,BQ),f32),pltpu.VMEM((E,BQ),f32),pltpu.VMEM((8,BQ),f32)],NEL*1024,prev)
def attn_bwd(h0,n,me,q,k,v,g,lse,prev):
    full,qblk,lblk=head_specs(h0)
    return attn_call(bwd_kernel,n,(me,q,k,v,g,lse),[qblk,full,full,full,lblk],
        pl.BlockSpec((3,1,E,T),lambda h,i,me:(0,h+h0,0,0)),jax.ShapeDtypeStruct((3,NH,E,T),bf16),
        [pltpu.VMEM((T,E),bf16),pltpu.VMEM((T,E),bf16),pltpu.VMEM((T,BQ),f32),pltpu.VMEM((T,BQ),f32),
         pltpu.VMEM((E,BQ),bf16),pltpu.VMEM((E,BQ),f32),pltpu.VMEM((E,T),f32),pltpu.VMEM((E,T),f32),pltpu.VMEM((8,BQ),f32)],NEL*2048,prev)

LN_EPS=1e-5
GELU_COEF=0.044715
GELU_SCALE=0.7978845608028654
D=2304
F=1152
ANY=pl.ANY

def send(a, pairs):
    return lax.ppermute(a, 'tp', pairs)
def partner(a): return send(a, [(i, i ^ 1) for i in range(8)])
def hop_a(a):
    return send(a, [(i, i ^ (2 if i % 2 == 0 else 4)) for i in range(8)])
def hop_b(a): return send(a, [(i, i ^ (4 if i % 2 == 0 else 2)) for i in range(8)])
def after(x, *deps): return lax.optimization_barrier((x,)+deps)[0]

def add2(a, b): return (a.astype(f32)+b.astype(f32)).astype(bf16)

def ln_fwd_kernel(rows, gain, bias, out):
    r=rows[...].astype(f32)
    cen=r-jnp.mean(r,axis=-1,keepdims=True)
    rstd=lax.rsqrt(jnp.mean(cen*cen,axis=-1,keepdims=True)+LN_EPS)
    out[...]=(cen*rstd*gain[...]+bias[...]).astype(bf16)

def layer_norm_fwd(rows, gain, bias):
    R=64
    blk=pl.BlockSpec((R,D),lambda i:(i,0)); vec=pl.BlockSpec((1,D),lambda i:(0,0))
    return pl.pallas_call(ln_fwd_kernel,grid=(256//R,),in_specs=[blk,vec,vec],out_specs=blk,out_shape=jax.ShapeDtypeStruct((256,D),bf16),
        compiler_params=pltpu.CompilerParams(dimension_semantics=("arbitrary",),vmem_limit_bytes=16<<20),
        cost_estimate=pl.CostEstimate(flops=256*D*1000,bytes_accessed=3<<20,transcendentals=0))(rows,gain.reshape(1,D),bias.reshape(1,D))

def ln_bwd_kernel(own, ro, a_in, *refs):
    rows, skip, gain, more, out, total, vec=refs[-7:]
    i=pl.program_id(0)
    b_in=refs[0][...].astype(f32) if len(refs)==8 else jnp.where(i<2,refs[0][...].astype(f32),refs[1][...].astype(f32))
    dh=(own[...].astype(f32)+ro[...].astype(f32))+(a_in[...].astype(f32)+b_in)
    r=rows[...].astype(f32)
    cen=r-jnp.mean(r,axis=-1,keepdims=True)
    rstd=lax.rsqrt(jnp.mean(cen*cen,axis=-1,keepdims=True)+LN_EPS)
    hat=cen*rstd
    gh=dh*gain[...]
    cg=gh-jnp.mean(gh,axis=-1,keepdims=True)
    sk=skip[...].astype(f32)
    o=(sk+rstd*(cg-hat*jnp.mean(gh*hat,axis=-1,keepdims=True))).astype(bf16)
    out[...]=o
    @pl.when(i==0)
    def _(): vec[...]=jnp.zeros_like(vec)
    vec[0]+=fold8(dh*hat); vec[1]+=fold8(dh)
    if total.shape[0]==4: vec[2]+=fold8(o.astype(f32)); vec[3]+=fold8(sk)
    @pl.when(i==3)
    def _():
        for k in range(2 if total.shape[0]==6 else 4): total[k:k+1,:]=jnp.sum(vec[k],axis=0,keepdims=True)
        if total.shape[0]==6: total[2:6,:]=more[...]

def ln_bwd(parts, rows, skip, gain, more):
    R=64
    blk=pl.BlockSpec((R,D),lambda i:(i,0))
    n=6 if more.shape[0]==4 else 4
    b_specs=[blk] if len(parts)==4 else [pl.BlockSpec((R,D),lambda i:(jnp.minimum(i,1),0)),pl.BlockSpec((R,D),lambda i:(jnp.maximum(i-2,0),0))]
    out,vec=pl.pallas_call(ln_bwd_kernel,grid=(256//R,),
        in_specs=[blk]*3+b_specs+[blk]*2+[pl.BlockSpec((1,D),lambda i:(0,0)),pl.BlockSpec(more.shape,lambda i:(0,0))],
        out_specs=[blk,pl.BlockSpec((n,D),lambda i:(0,0))],scratch_shapes=[pltpu.VMEM((4,8,D),f32)],
        out_shape=[jax.ShapeDtypeStruct((256,D),bf16),jax.ShapeDtypeStruct((n,D),f32)],
        compiler_params=pltpu.CompilerParams(dimension_semantics=("arbitrary",),vmem_limit_bytes=16<<20),
        cost_estimate=pl.CostEstimate(flops=256*D*1000,bytes_accessed=6<<20,transcendentals=0))(*parts,rows,skip,gain.reshape(1,D),more)
    return out,vec

def join(a, b):
    def kernel(a, b, out):
        out[0]=a[0]; out[1]=b[0]
    return pl.pallas_call(kernel,name="lse_join",out_shape=jax.ShapeDtypeStruct((2,1,T),f32),compiler_params=pltpu.CompilerParams(vmem_limit_bytes=4<<20),
        cost_estimate=pl.CostEstimate(flops=T*100,bytes_accessed=8*T,transcendentals=0))(a,b)

def call(kernel, grid, in_specs, out_specs, out_shape, scratch, flops, args):
    return pl.pallas_call(kernel,grid=grid,in_specs=in_specs,out_specs=out_specs,out_shape=out_shape,
        scratch_shapes=scratch,compiler_params=pltpu.CompilerParams(dimension_semantics=("arbitrary",)*len(grid),vmem_limit_bytes=24<<20),
        cost_estimate=pl.CostEstimate(flops=flops,bytes_accessed=30<<20,transcendentals=0))(*args)

RB=256; SUB=BLK//RB
def mlp(first, blk, pieces, z, w2, w1, prev):
    n=len(pieces)//2
    def kernel(*refs):
        dy=refs[1:1+2*n]; z_ref,w2h,w1h=refs[1+2*n:4+2*n]
        refs=refs[2*n+(4 if prev is None else 6):]
        dz_ref,u_ref,db_ref=refs[:3]; dh=refs[3:3+2*n]
        x,w2s,w1s,st,xsem,wsem,osem=refs[3+2*n:]
        s=pl.program_id(0)
        class wcopy:
            def __init__(self, k):
                h,v=((w2h,w2s),(w1h,w1s))[k]
                r=v.shape[0]//4
                self.cs=[pltpu.make_async_copy(h.at[j*r:(j+1)*r],v.at[j*r:(j+1)*r],wsem.at[k,j]) for j in range(4)]
            def start(self):
                for c in self.cs: c.start()
            def wait(self):
                for c in self.cs: c.wait()
        def xcopy(p): return pltpu.make_async_copy(dy[p],x.at[p*BLK:(p+1)*BLK],xsem.at[p])
        def ocopy(p): return pltpu.make_async_copy(st.at[p*BLK:(p+1)*BLK],dh[p],osem.at[p])
        @pl.when(s==0)
        def _():
            xcopy(0).start()
            wcopy(0).start()
            for p in range(1,2*n): xcopy(p).start()
            wcopy(1).start()
            db_ref[...]=jnp.zeros_like(db_ref)
            wcopy(0).wait()
        for k in range(2*n):
            @pl.when(s==k*SUB)
            def _(): xcopy(k).wait()
        rows=pl.ds(pl.multiple_of(s*RB,RB),RB)
        zf=z_ref[...].astype(f32)
        t=zf*zf
        th=jnp.tanh(zf*(GELU_SCALE*GELU_COEF*t+GELU_SCALE))
        hz=0.5*zf
        u_ref[...]=(hz*th+hz).astype(bf16)
        slope=(0.5*th+0.5)+hz*(1.0-th*th)*(3.0*GELU_SCALE*GELU_COEF*t+GELU_SCALE)
        dz=(tn(x[rows,:],w2s[...],1,1)*slope).astype(bf16)
        dz_ref[...]=dz
        db_ref[...]+=fold8(dz.astype(f32))
        @pl.when(s==0)
        def _(): wcopy(1).wait()
        if first==1: st[rows,:]=tn(dz_ref[...],w1s[...],1,1).astype(bf16)
        else:
            def part(c,_):
                at=pl.ds(pl.multiple_of(c*768,768),768)
                st[rows,at]=tn(dz_ref[...],w1s[at,:],1,1).astype(bf16)
                return 0
            lax.fori_loop(0,3,part,0)
        for k in range(2*n):
            @pl.when(s==k*SUB+SUB-1)
            def _(): ocopy(k).start()
        @pl.when(s==2*n*SUB-1)
        def _():
            for p in range(2*n): ocopy(p).wait()
    any_=pl.BlockSpec(memory_space=ANY)
    step=pl.BlockSpec((RB,F),lambda s,blk:(s+2*first*SUB,0))
    extra=() if prev is None else prev
    outs=pl.pallas_call(kernel,
        grid_spec=pltpu.PrefetchScalarGridSpec(num_scalar_prefetch=1,grid=(2*n*SUB,),
            in_specs=[any_]*(2*n)+[pl.BlockSpec((RB,F),lambda s,blk:(blk[s//SUB+2*first]*SUB+s%SUB,0))]+[any_]*(2+len(extra)),
            out_specs=[step,step,pl.BlockSpec((8,F),lambda s,blk:(0,0))]+[any_]*(2*n),
            scratch_shapes=[pltpu.VMEM((2*n*BLK,D),bf16),pltpu.VMEM((F,D),bf16),pltpu.VMEM((D,F),bf16),pltpu.VMEM((2*n*BLK,D),bf16),
             pltpu.SemaphoreType.DMA((2*n,)),pltpu.SemaphoreType.DMA((2,4)),pltpu.SemaphoreType.DMA((2*n,))]),
        out_shape=[jax.ShapeDtypeStruct((T,F),bf16)]*2+[jax.ShapeDtypeStruct((8,F),f32)]+[jax.ShapeDtypeStruct((BLK,D),bf16)]*(2*n),
        input_output_aliases={2*n+4+k:k for k in range(len(extra))},
        compiler_params=pltpu.CompilerParams(dimension_semantics=("arbitrary",),vmem_limit_bytes=48<<20),
        cost_estimate=pl.CostEstimate(flops=n*T*D*F,bytes_accessed=20<<20,transcendentals=0))(blk,*pieces,z,w2,w1,*extra)
    return (outs[0],outs[1]),outs[2],list(outs[3:])

def attn_in_grad(chips, dqkv, wqkv):
    c0,c1=chips
    def kernel(g,w,*refs):
        dh=refs[:4]; st,sem=refs[4:]
        s=pl.program_id(0)
        def ocopy(p): return pltpu.make_async_copy(st.at[p*BLK:(p+1)*BLK],dh[p],sem.at[p])
        rows=pl.ds(pl.multiple_of(s*BLK,BLK),BLK)
        st[rows,:]=tn(g[...],w[...],0,0).astype(bf16)
        for k in range(4):
            @pl.when(s==k)
            def _(): ocopy(k).start()
        @pl.when(s==3)
        def _():
            for p in range(4): ocopy(p).wait()
    K=3*NH*E
    return call(kernel,(4,),[pl.BlockSpec((K,BLK),lambda s:(0,2*(c0+(c1-c0)*(s//2))+s%2)),pl.BlockSpec((K,D),lambda s:(0,0))],
        [pl.BlockSpec(memory_space=ANY)]*4,[jax.ShapeDtypeStruct((BLK,D),bf16)]*4,
        [pltpu.VMEM((4*BLK,D),bf16),pltpu.SemaphoreType.DMA((4,))],T*D*K,(dqkv,wqkv))

def gathered_mm(body, pieces, other, n, out_spec, out_shape, flops, cols=(0,D), into=None, vmem=60):
    W=(cols[1]-cols[0])//n
    def kernel(*refs):
        ps=refs[:8]; o_ref=refs[8]; out,full,sem=refs[-3:]
        s=pl.program_id(0)
        def copy(t,p): return pltpu.make_async_copy(ps[p].at[:,cols[0]+t*W:cols[0]+(t+1)*W],full.at[t,p*BLK:(p+1)*BLK],sem.at[t,p])
        @pl.when(s==0)
        def _():
            for t in range(n):
                for p in range(8): copy(t,p).start()
        for t in range(n):
            @pl.when(s==t)
            def _():
                for p in range(8): copy(t,p).wait()
        out[...]=body(full[s],o_ref)
    any_=pl.BlockSpec(memory_space=ANY)
    extra=() if into is None else (into,)
    return pl.pallas_call(kernel,grid=(n,),in_specs=[any_]*8+[pl.BlockSpec(other.shape,lambda s:(0,0))]+[any_]*len(extra),out_specs=out_spec,out_shape=out_shape,
        scratch_shapes=[pltpu.VMEM((n,T,W),bf16),pltpu.SemaphoreType.DMA((n,8))],input_output_aliases={9:0} if extra else {},
        compiler_params=pltpu.CompilerParams(dimension_semantics=("arbitrary",),vmem_limit_bytes=vmem<<20),
        cost_estimate=pl.CostEstimate(flops=flops,bytes_accessed=30<<20,transcendentals=0))(*pieces,other,*extra)

def ctx_grad(first, pieces, wo, into):
    n=len(pieces)//2
    def kernel(*refs):
        ps=refs[:2*n]; w=refs[2*n]; out,full,sem=refs[-3:]
        s=pl.program_id(0)
        def copy(p): return pltpu.make_async_copy(ps[p],full.at[p//2,(p%2)*BLK:(p%2+1)*BLK],sem.at[p])
        @pl.when(s==0)
        def _():
            for p in range(2*n): copy(p).start()
        for k in range(n):
            @pl.when(s==k)
            def _():
                copy(2*k).wait(); copy(2*k+1).wait()
        out[...]=tn(w[...],full[s],1,1).astype(bf16)
    any_=pl.BlockSpec(memory_space=ANY)
    extra=() if into is None else (into,)
    return pl.pallas_call(kernel,grid=(n,),in_specs=[any_]*(2*n)+[pl.BlockSpec((NH*E,D),lambda s:(0,0))]+[any_]*len(extra),
        out_specs=pl.BlockSpec((NH*E,2*BLK),lambda s:(0,s+first)),out_shape=jax.ShapeDtypeStruct((NH*E,T),bf16),
        scratch_shapes=[pltpu.VMEM((n,2*BLK,D),bf16),pltpu.SemaphoreType.DMA((2*n,))],input_output_aliases={2*n+1:0} if extra else {},
        compiler_params=pltpu.CompilerParams(dimension_semantics=("arbitrary",),vmem_limit_bytes=24<<20),
        cost_estimate=pl.CostEstimate(flops=n*512*D*NH*E*2,bytes_accessed=10<<20,transcendentals=0))(*pieces,wo,*extra)

def solution(mesh):
    def layer(x_in, x_mid, d_out, q_saved, k_saved, v_saved, z_saved, g1, b1, g2, b2, w_qkv, w_proj, w_fc1, w_fc2):
        me=lax.axis_index('tp').astype(jnp.int32)
        me1=jnp.reshape(me,(1,))
        p8=jnp.arange(8,dtype=jnp.int32)
        blk=lax.bitwise_xor(me,2*turn(p8//2,me%2)+p8%2)
        x_in, x_mid, d_out, z = x_in[0], x_mid[0], d_out[0], z_saved[0]
        heads=lambda a: a[0].transpose(1,2,0)
        q,k,v=heads(q_saved),heads(k_saved),heads(v_saved)
        wqkv=w_qkv.transpose(0,2,3,1).reshape(3*NH*E,D)
        wo=w_proj.reshape(NH*E,D)
        dya,dyb,dyp=hop_a(d_out),hop_b(d_out),partner(d_out)
        dzu,db_0,(o0,o1)=mlp(0,blk,[d_out,dyp],z,w_fc2,w_fc1,None)
        h2_local=layer_norm_fwd(after(x_mid,db_0),g2,b2)
        dya=after(dya,db_0,h2_local)
        dyd=hop_b(dya)
        h2_local=after(h2_local,dya)
        h2a,h2b,h2p=hop_a(h2_local),hop_b(h2_local),partner(h2_local)
        dypa,dypb=partner(dya),partner(dyb)
        dzu,db_1,(pa0,pa1,pb0,pb1)=mlp(1,blk,[dya,dypb,dyb,dypa],z,w_fc2,w_fc1,dzu)
        ra,rb,ro=partner(pb1),partner(pa1),partner(o1)
        h1_local=layer_norm_fwd(after(x_in,db_1),g1,b1)
        a_in=hop_a(add2(pa0,ra))
        dypd=partner(dyd)
        (dz,u),db_2,(pd0,pd1)=mlp(3,blk,[dyd,dypd],z,w_fc2,w_fc1,dzu)
        rd=partner(pd1)
        d_sum=[add2(pd0[:128],rd[:128]),add2(pd0[128:],rd[128:])]
        d_in=[hop_a(d_sum[0]),hop_a(d_sum[1])]
        def b_half(k,lse): return (pb0[128*k:128*k+128].astype(f32)+after(rb,lse)[128*k:128*k+128].astype(f32)+d_in[k].astype(f32)).astype(bf16)
        ctx,lse0=attn_fwd(0,1,me1,after(q,*d_sum),k,v,None)
        b_sum=b_half(0,lse0)
        b_in0=hop_b(b_sum)
        ctx,lse1=attn_fwd(1,1,me1,after(q,b_sum),k,v,ctx)
        b_sum=b_half(1,lse1)
        b_in1=hop_b(b_sum)
        ctx,lse2=attn_fwd(2,1,me1,after(q,b_sum),k,v,ctx)
        h2a=after(h2a,b_sum)
        h2d=hop_b(h2a); h2pa,h2pb=partner(h2a),partner(h2b)
        mid,vec2=ln_bwd((after(o0,lse2),ro,a_in,b_in0,b_in1),x_mid,d_out,g2,g2.reshape(1,D))
        grad_bfc1=jnp.sum(db_0+db_1+db_2,axis=0)
        dxa,dxb,dxp=hop_a(mid),hop_b(mid),partner(mid)
        dys=[d_out,dyp,dya,dypb,dyb,dypa,dyd,dypd]
        grad_wfc2=gathered_mm(lambda x,o: tn(o[...],x,0,0),dys,after(u,mid),9,
            pl.BlockSpec((F,256),lambda s:(0,s)),jax.ShapeDtypeStruct((F,D),f32),2*T*D*F,vmem=60)
        h2pd=partner(after(h2d,grad_wfc2))
        h2=[h2_local,h2p,h2a,h2pb,h2b,h2pa,h2d,h2pd]
        lse01=join(after(lse0,grad_wfc2),lse1)
        def w1_part(c0,n,left,into):
            return gathered_mm(lambda x,o: tn(x,o[...],0,0),h2,left,n,
                pl.BlockSpec((256,F),lambda s:(s+c0,0)),jax.ShapeDtypeStruct((D,F),f32),2*T*256*n*F,cols=(256*c0,256*(c0+n)),into=into,vmem=26)
        grad_wfc1=w1_part(0,3,after(dz,grad_wfc2),None)
        dxa=after(dxa,grad_wfc1)
        dxd=hop_b(dxa)
        dxpa,dxpb=partner(dxa),partner(dxb)
        grad_wfc1=w1_part(3,6,after(dz,dxa),grad_wfc1)
        dctx=ctx_grad(0,[mid,dxp,dxa,dxpb,dxb,dxpa],after(wo,grad_wfc1),None)
        dxd=after(dxd,dctx)
        dxpd=partner(dxd)
        h1_local=after(h1_local,dxd)
        h1a,h1b,h1p=hop_a(h1_local),hop_b(h1_local),partner(h1_local)
        dx1=[mid,dxp,dxa,dxpb,dxb,dxpa,dxd,dxpd]
        dctx=ctx_grad(3,[dxd,dxpd],wo,dctx).reshape(NH,E,T)
        dqkv=attn_bwd(0,2,me1,q,k,v,dctx,lse01,None)
        h1a=after(h1a,dqkv)
        h1d=hop_b(h1a); h1pa,h1pb=partner(h1a),partner(h1b)
        dqkv=attn_bwd(2,1,me1,q,k,v,dctx,lse2,dqkv)
        dqkv=dqkv.reshape(3*NH*E,T)
        grad_bqkv=jnp.sum(dqkv,axis=1,dtype=f32).reshape(3,NH,E)
        pd0,pd1,pa0,pa1=attn_in_grad((3,1),dqkv,wqkv)
        d_sum=add2(pd0,partner(pd1))
        d_in=hop_a(d_sum)
        rb=partner(pa1)
        pb0,pb1,o0,o1=attn_in_grad((2,0),after(dqkv,d_sum),wqkv)
        ra,ro=partner(pb1),partner(o1)
        a_sum=add2(pa0,ra)
        a_in=hop_a(a_sum)
        b_sum=(pb0.astype(f32)+after(rb,a_sum).astype(f32)+d_in.astype(f32)).astype(bf16)
        b_in=hop_b(b_sum)
        h1pd=partner(after(h1d,dqkv))
        h1=[h1_local,h1p,h1a,h1pb,h1b,h1pa,h1d,h1pd]
        grad_wqkv=gathered_mm(lambda x,o: jnp.dot(o[...],x,preferred_element_type=f32),h1,after(dqkv,b_sum),3,
            pl.BlockSpec((3*NH*E,768),lambda s:(0,s)),jax.ShapeDtypeStruct((3*NH*E,D),f32),6*T*D*NH*E,vmem=30)
        def wo_part(c0,n,left,into):
            return gathered_mm(lambda x,o: jnp.dot(o[...],x,preferred_element_type=f32),dx1,left,n,
                pl.BlockSpec((NH*E,256),lambda s:(0,s+c0)),jax.ShapeDtypeStruct((NH*E,D),f32),n*T*256*NH*E*2,cols=(256*c0,256*(c0+n)),into=into,vmem=14)
        ctx=ctx.reshape(NH*E,T)
        grad_wproj=wo_part(0,6,after(ctx,grad_wqkv),None)
        dx,grad_vecs=ln_bwd((after(o0,grad_wproj),ro,a_in,b_in),x_in,mid,g1,vec2)
        v2,v4,v6=(send(grad_vecs,[(i,i^k) for i in range(8)]) for k in (2,4,6))
        grad_wproj=wo_part(6,3,after(ctx,dx),grad_wproj)
        vecs=(grad_vecs+after(v2,grad_wproj))+(v4+v6)
        v1=send(vecs,[(i,i^1) for i in range(8)])
        grad_vecs=vecs+v1
        grad_wproj=grad_wproj.reshape(NH,E,D)
        grad_wqkv=grad_wqkv.reshape(3,NH,E,D).transpose(0,3,1,2)
        return dx[None], grad_wqkv, grad_bqkv, grad_wproj, grad_wfc1, grad_bfc1, grad_wfc2, grad_vecs

    tok_spec = P('dp', 'tp', None)
    head_spec = P('dp', None, 'tp', None)
    in_specs = (tok_spec, tok_spec, tok_spec, head_spec, head_spec, head_spec, P('dp', None, 'tp'),
                P(None), P(None), P(None), P(None),
                P(None, None, 'tp', None), P('tp', None, None), P(None, 'tp'), P('tp', None))
    out_specs = (tok_spec, P('dp', None, 'tp', None), P('dp', 'tp', None), P(('dp', 'tp'), None, None),
                 P('dp', 'tp'), P(('dp', 'tp')), P(('dp', 'tp'), None), P('dp', None))
    return jax.shard_map(layer, mesh=mesh, in_specs=in_specs, out_specs=out_specs, check_vma=False)
```
